16 devices in a mesh: dp: 4 (over z, y), stage: 4 (over x, core).
Axes of the slice: x: 2, y: 2, z: 2, core: 2. Of those that a mesh axis runs over, the one named last changes fastest.
Arguments:
- tokens_in: bfloat16 [128, 256, 512], P('dp'), parts along dimension 0
- targets: bfloat16 [128, 256, 512], P('dp'), parts along dimension 0
- w_in: bfloat16 [8, 512, 2048], P('stage')
- w_out: bfloat16 [8, 2048, 512], P('stage')
- norm_gains: float32 [8, 512], P('stage')
Outputs:
- output 1: float32 [32, 512, 2048], P(('dp', 'stage')), parts along dimension 0
- output 2: float32 [32, 2048, 512], P(('dp', 'stage')), parts along dimension 0
- output 3: float32 [32, 512], P(('dp', 'stage')), parts along dimension 0
- output 4: float32 [4], P('dp'), parts along dimension 0
There are 4 independent parts. The reference program is written for one: setup_inputs(seed, part) draws one part's arguments, and reference() takes and returns one part's arrays. A program takes and returns all parts, laid end to end along the dimension named above; an argument that names none is the same for every part.
All inputs are finite; a program needn't handle non-finite values.
Results may differ from the reference program's by a relative error of at most 0.00280117.
Values are sent between devices in bfloat16 or wider.
A program may use at most 1 GiB of HBM per device.

```python
import jax
import jax.numpy as jnp
from jax import lax

STAGES = 4
SEGMENT_LAYERS = 1
MICRO_BATCHES = 32
MICRO_TOKENS = 256
D_MODEL = 512
D_FF = 2048
LAYERS = 2 * STAGES * SEGMENT_LAYERS
EPSILON = 1e-6


def setup_inputs(seed: int = 0, part: int = 0) -> dict:
    base_key = jax.random.key(seed)
    key_list = jax.random.split(base_key, 4)
    data_key = jax.random.fold_in(key_list[0], part)
    key_tokens, key_targets = jax.random.split(data_key)
    shape_act = (MICRO_BATCHES, MICRO_TOKENS, D_MODEL)
    target_scale = (1.0 + 0.5 * LAYERS) ** 0.5
    tokens_in = jax.random.normal(key_tokens, shape_act, jnp.float32)
    targets = target_scale * jax.random.normal(key_targets, shape_act, jnp.float32)
    w_in = jax.random.normal(key_list[1], (LAYERS, D_MODEL, D_FF), jnp.float32) * D_MODEL ** -0.5
    w_out = jax.random.normal(key_list[2], (LAYERS, D_FF, D_MODEL), jnp.float32) * D_FF ** -0.5
    norm_gains = 1.0 + 0.5 * jax.random.normal(key_list[3], (LAYERS, D_MODEL), jnp.float32)
    return {
        'tokens_in': tokens_in.astype(jnp.bfloat16),
        'targets': targets.astype(jnp.bfloat16),
        'w_in': w_in.astype(jnp.bfloat16),
        'w_out': w_out.astype(jnp.bfloat16),
        'norm_gains': norm_gains,
    }


def norm_scale(x_f32, gain_vec):
    inv_rms = lax.rsqrt(jnp.mean(x_f32 * x_f32, axis=-1, keepdims=True) + EPSILON)
    return x_f32 * inv_rms * gain_vec


def layer_forward(x_act, first_w, second_w, gain_vec):
    x_f32 = x_act.astype(jnp.float32)
    normed = norm_scale(x_f32, gain_vec).astype(jnp.bfloat16)
    pre_act = jnp.dot(normed, first_w, preferred_element_type=jnp.float32)
    hidden = jax.nn.gelu(pre_act).astype(jnp.bfloat16)
    out_f32 = jnp.dot(hidden, second_w, preferred_element_type=jnp.float32)
    return (x_f32 + out_f32).astype(jnp.bfloat16)


def layer_backward(x_act, grad_h, first_w, second_w, gain_vec):
    x_f32 = x_act.astype(jnp.float32)
    normed_f32, norm_vjp = jax.vjp(norm_scale, x_f32, gain_vec)
    normed = normed_f32.astype(jnp.bfloat16)
    pre_act = jnp.dot(normed, first_w, preferred_element_type=jnp.float32)
    hidden_f32, gelu_vjp = jax.vjp(jax.nn.gelu, pre_act)
    hidden = hidden_f32.astype(jnp.bfloat16)
    grad_second = jnp.dot(hidden.T, grad_h, preferred_element_type=jnp.float32)
    grad_hidden = jnp.dot(grad_h, second_w.T, preferred_element_type=jnp.float32)
    grad_pre = gelu_vjp(grad_hidden)[0].astype(jnp.bfloat16)
    grad_first = jnp.dot(normed.T, grad_pre, preferred_element_type=jnp.float32)
    grad_normed = jnp.dot(grad_pre, first_w.T, preferred_element_type=jnp.float32)
    grad_x_norm, grad_gain = norm_vjp(grad_normed)
    grad_x = (grad_h.astype(jnp.float32) + grad_x_norm).astype(jnp.bfloat16)
    return grad_x, grad_first, grad_second, grad_gain


def to_exec_order(stored):
    tail_shape = stored.shape[1:]
    blocks = stored.reshape((STAGES, 2, SEGMENT_LAYERS) + tail_shape)
    down_half = blocks[:, 0].reshape((STAGES * SEGMENT_LAYERS,) + tail_shape)
    up_half = blocks[::-1, 1].reshape((STAGES * SEGMENT_LAYERS,) + tail_shape)
    return jnp.concatenate([down_half, up_half], axis=0)


def to_stored_order(in_exec):
    tail_shape = in_exec.shape[1:]
    half_rows = STAGES * SEGMENT_LAYERS
    down_half = in_exec[:half_rows].reshape((STAGES, SEGMENT_LAYERS) + tail_shape)
    up_half = in_exec[half_rows:].reshape((STAGES, SEGMENT_LAYERS) + tail_shape)[::-1]
    return jnp.stack([down_half, up_half], axis=1).reshape((LAYERS,) + tail_shape)


def reference(tokens_in, targets, w_in, w_out, norm_gains):
    first_all = to_exec_order(w_in)
    second_all = to_exec_order(w_out)
    gain_all = to_exec_order(norm_gains)
    seed_scale = 2.0 / (MICRO_BATCHES * MICRO_TOKENS)

    def micro_step(loop_state, micro_pair):
        sum_first, sum_second, sum_gain, sse_total = loop_state
        micro_tokens, micro_targets = micro_pair

        def forward_layer(act_in, layer_weights):
            return layer_forward(act_in, layer_weights[0], layer_weights[1], layer_weights[2]), act_in

        final_act, saved_inputs = lax.scan(forward_layer, micro_tokens, (first_all, second_all, gain_all))
        error_f32 = final_act.astype(jnp.float32) - micro_targets.astype(jnp.float32)
        seed_grad = (error_f32 * seed_scale).astype(jnp.bfloat16)

        def backward_layer(grad_h, layer_data):
            grad_x, grad_first, grad_second, grad_gain = layer_backward(
                layer_data[0], grad_h, layer_data[1], layer_data[2], layer_data[3])
            return grad_x, (grad_first, grad_second, grad_gain)

        _, layer_grads = lax.scan(backward_layer, seed_grad,
                                  (saved_inputs, first_all, second_all, gain_all), reverse=True)
        new_state = (sum_first + layer_grads[0], sum_second + layer_grads[1],
                     sum_gain + layer_grads[2], sse_total + jnp.sum(error_f32 * error_f32))
        return new_state, None

    init_state = (jnp.zeros((LAYERS, D_MODEL, D_FF), jnp.float32),
                  jnp.zeros((LAYERS, D_FF, D_MODEL), jnp.float32),
                  jnp.zeros((LAYERS, D_MODEL), jnp.float32),
                  jnp.zeros((), jnp.float32))
    final_state, _ = lax.scan(micro_step, init_state, (tokens_in, targets))
    loss_value = final_state[3] / (MICRO_BATCHES * MICRO_TOKENS * D_MODEL)
    return (to_stored_order(final_state[0]), to_stored_order(final_state[1]),
            to_stored_order(final_state[2]), loss_value.reshape(1))
```

```python
import functools

import jax
import jax.numpy as jnp
from jax import lax
from jax.experimental import pallas as pl
from jax.experimental.pallas import tpu as pltpu
from jax.sharding import PartitionSpec as P

EPSILON = 1e-6
MESH = pl.DeviceIdType.MESH
F32 = jnp.float32
BF16 = jnp.bfloat16
C0 = 0.7978845608028654
C1 = C0 * 0.044715
RING = 8
TOK_AHEAD = 4
TGT_SLOTS = 4
CHUNK_F = 512
CHUNK_B = 512


def dot(lhs, rhs):
    return jnp.dot(lhs, rhs, preferred_element_type=F32)


def dot_t(lhs, rhs):
    return lax.dot_general(lhs, rhs, (((1,), (1,)), ((), ())), preferred_element_type=F32)


def gate(a):
    sq = a * a
    z = a * (C0 + C1 * sq)
    return 0.5 + 0.5 * jnp.tanh(z), sq


def kernel(n_stage, n_micro, tok_hbm, tgt_hbm, wi_hbm, wo_hbm, gain_ref,
           gwi_hbm, gwo_hbm, gg_ref, loss_ref,
           wi, wo, agi, ago, gg, xs, dhs, of, ob, tg, da_s, u_s, sse, loss_src, loss_dst,
           w_sem, out_sem, tg_sem, rx_sem, rd_sem, sf_sem, sb_sem, free_sem, lsend_sem, lrecv_sem):
    stage = lax.axis_index('stage')
    last = n_stage - 1
    is_first = stage == 0
    is_last = stage == last
    tokens_mb, d_model = xs.shape[2], xs.shape[3]
    d_ff = wi.shape[2]
    seed_scale = 2.0 / (n_micro * tokens_mb)

    barrier = pltpu.get_barrier_semaphore()
    for hop in range(1, n_stage):
        pl.semaphore_signal(barrier, inc=1, device_id={'stage': lax.rem(stage + hop, n_stage)},
                            device_id_type=MESH)
    pl.semaphore_wait(barrier, n_stage - 1)

    def weight_copies(layer):
        return (pltpu.make_async_copy(wi_hbm.at[layer], wi.at[layer], w_sem.at[layer, 0]),
                pltpu.make_async_copy(wo_hbm.at[layer], wo.at[layer], w_sem.at[layer, 1]))

    def token_copy(mb):
        return pltpu.make_async_copy(tok_hbm.at[mb], xs.at[0, mb], rx_sem.at[0, mb])

    def target_copy(mb):
        slot = lax.rem(mb, TGT_SLOTS)
        return pltpu.make_async_copy(tgt_hbm.at[mb], tg.at[slot], tg_sem.at[slot])

    def out_copies(layer):
        return (pltpu.make_async_copy(agi.at[layer], gwi_hbm.at[layer], out_sem.at[layer, 0]),
                pltpu.make_async_copy(ago.at[layer], gwo_hbm.at[layer], out_sem.at[layer, 1]))

    for copy in weight_copies(0):
        copy.start()

    @pl.when(is_first)
    def _():
        for mb in range(TOK_AHEAD):
            token_copy(mb).start()

    for copy in weight_copies(1):
        copy.start()

    @pl.when(is_first)
    def _():
        for mb in range(TGT_SLOTS):
            target_copy(mb).start()

    @pl.loop(0, 2 * d_model // 8)
    def _(i):
        layer, row = i // (d_model // 8), lax.rem(i, d_model // 8)
        rows = pl.ds(pl.multiple_of(row * 8, 8), 8)
        agi[layer, rows, :] = jnp.zeros((8, d_ff), F32)
        ago[layer, rows, :] = jnp.zeros((8, d_ff), F32)

    gg[...] = jnp.zeros_like(gg)
    sse[...] = jnp.zeros_like(sse)
    for layer in range(2):
        for copy in weight_copies(layer):
            copy.wait()

    def gain_of(layer):
        return jnp.where(layer == 0, gain_ref[0:1, :], gain_ref[1:2, :])

    def fold(rows):
        return jnp.sum(rows.reshape(rows.shape[0] // 8, 8, rows.shape[1]), axis=0)

    def forward(layer, mb):
        x = xs[layer, mb].astype(F32)
        inv = lax.rsqrt(jnp.mean(x * x, axis=-1, keepdims=True) + EPSILON)
        normed = (x * inv * gain_of(layer)).astype(BF16)
        total = x
        for c in range(d_ff // CHUNK_F):
            cols = pl.ds(c * CHUNK_F, CHUNK_F)
            a = dot(normed, wi[layer, :, cols])
            q, _ = gate(a)
            total = total + dot((a * q).astype(BF16), wo[layer, cols, :])
        return total.astype(BF16)

    def backward(layer, mb, slot):
        x = xs[layer, mb].astype(F32)
        gain = gain_of(layer)
        inv = lax.rsqrt(jnp.mean(x * x, axis=-1, keepdims=True) + EPSILON)
        xhat = x * inv
        normed = (xhat * gain).astype(BF16)
        dh = dhs[layer, slot]
        dn = None
        for c in range(d_ff // CHUNK_B):
            cols = pl.ds(c * CHUNK_B, CHUNK_B)
            a = dot(normed, wi[layer, :, cols])
            du = dot_t(dh, wo[layer, cols, :])
            q, sq = gate(a)
            u = a * q
            slope = q + u * (1.0 - q) * (2.0 * C0 + 6.0 * C1 * sq)
            da = (du * slope).astype(BF16)
            u_s[:, cols] = u.astype(BF16)
            da_s[:, cols] = da
            part = dot_t(da, wi[layer, :, cols])
            dn = part if dn is None else dn + part
        weighted = dn * gain
        proj = jnp.mean(weighted * xhat, axis=-1, keepdims=True)
        gg[layer] += fold(dn * xhat)
        return (dh.astype(F32) + inv * (weighted - xhat * proj)).astype(BF16)

    def weight_grads(layer, mb, slot):
        x = xs[layer, mb].astype(F32)
        inv = lax.rsqrt(jnp.mean(x * x, axis=-1, keepdims=True) + EPSILON)
        normed_t = (x * inv * gain_of(layer)).astype(BF16).T
        dh_t = dhs[layer, slot].T
        for c in range(d_ff // CHUNK_B):
            cols = pl.ds(c * CHUNK_B, CHUNK_B)
            agi[layer, :, cols] += dot(normed_t, da_s[:, cols])
            ago[layer, :, cols] += dot(dh_t, u_s[:, cols])

    def send_f(layer, mb, target):
        par = lax.rem(mb, 2)
        return pltpu.make_async_remote_copy(
            src_ref=of.at[layer, par], dst_ref=xs.at[layer, mb],
            send_sem=sf_sem.at[layer, par], recv_sem=rx_sem.at[layer, mb],
            device_id={'stage': target}, device_id_type=MESH)

    def send_b(layer, mb, target):
        par = lax.rem(mb, 2)
        slot = lax.rem(mb, RING)
        return pltpu.make_async_remote_copy(
            src_ref=ob.at[layer, par], dst_ref=dhs.at[layer, slot],
            send_sem=sb_sem.at[layer, par], recv_sem=rd_sem.at[layer, slot],
            device_id={'stage': target}, device_id_type=MESH)

    def forward_unit(layer, mb):
        down = layer == 0
        sends = jnp.where(down, stage < last, stage > 0)
        receives = jnp.where(down, True, stage < last)
        target = jnp.where(down, jnp.minimum(stage + 1, last), jnp.maximum(stage - 1, 0))
        par = lax.rem(mb, 2)

        @pl.when(down & is_first & (mb + TOK_AHEAD < n_micro))
        def _():
            token_copy(mb + TOK_AHEAD).start()

        @pl.when(receives)
        def _():
            send_f(layer, mb, target).wait_recv()

        @pl.when(sends & (mb >= 2))
        def _():
            send_f(layer, mb - 2, target).wait_send()

        of[layer, par] = forward(layer, mb)

        @pl.when(sends)
        def _():
            send_f(layer, mb, target).start()

        @pl.when(down & is_last)
        def _():
            xs[1, mb] = of[0, par]

        @pl.when(jnp.logical_not(down) & is_first)
        def _():
            target_copy(mb).wait()
            tslot = lax.rem(mb, TGT_SLOTS)
            err = of[1, par].astype(F32) - tg[tslot].astype(F32)
            dhs[1, lax.rem(mb, RING)] = (err * seed_scale).astype(BF16)
            sse[...] += fold(err * err)

            @pl.when(mb + TGT_SLOTS < n_micro)
            def _():
                target_copy(mb + TGT_SLOTS).start()

    def backward_unit(layer, mb):
        up = layer == 1
        sends = jnp.where(up, stage < last, stage > 0)
        receives = jnp.where(up, stage > 0, stage < last)
        target = jnp.where(up, jnp.minimum(stage + 1, last), jnp.maximum(stage - 1, 0))
        source = jnp.where(up, jnp.maximum(stage - 1, 0), jnp.minimum(stage + 1, last))
        par = lax.rem(mb, 2)
        slot = lax.rem(mb, RING)

        @pl.when(receives)
        def _():
            send_b(layer, mb, target).wait_recv()

        @pl.when(sends & (mb >= 2))
        def _():
            send_b(layer, mb - 2, target).wait_send()

        ob[layer, par] = backward(layer, mb, slot)

        @pl.when(sends & (mb >= RING))
        def _():
            pl.semaphore_wait(free_sem.at[layer], 1)

        @pl.when(sends)
        def _():
            send_b(layer, mb, target).start()

        @pl.when(up & is_last)
        def _():
            dhs[0, slot] = ob[1, par]

        weight_grads(layer, mb, slot)

        @pl.when(receives & (mb + RING < n_micro))
        def _():
            pl.semaphore_signal(free_sem.at[layer], inc=1, device_id={'stage': source}, device_id_type=MESH)

        @pl.when(mb == n_micro - 1)
        def _():
            for copy in out_copies(layer):
                copy.start()

    def loss_copy(peer):
        return pltpu.make_async_remote_copy(
            src_ref=loss_src, dst_ref=loss_dst, send_sem=lsend_sem.at[peer - 1], recv_sem=lrecv_sem.at[0],
            device_id={'stage': peer}, device_id_type=MESH)

    ticks = n_micro + 4 * last

    @pl.loop(0, ticks)
    def _(tick):
        @pl.loop(0, 2)
        def _(layer):
            mb = tick - jnp.where(layer == 0, stage, 2 * last - stage)

            @pl.when((mb >= 0) & (mb < n_micro))
            def _():
                forward_unit(layer, mb)

        @pl.when(is_first & (tick == n_micro - 1 + 2 * last))
        def _():
            total = jnp.sum(sse[...]) / (n_micro * tokens_mb * d_model)
            loss_src[...] = jnp.full(loss_src.shape, total, F32)
            for peer in range(1, n_stage):
                loss_copy(peer).start()

        @pl.loop(0, 2)
        def _(index):
            layer = 1 - index
            mb = tick - jnp.where(layer == 1, 2 * last + stage, 4 * last - stage)

            @pl.when((mb >= 0) & (mb < n_micro))
            def _():
                backward_unit(layer, mb)

    gg_ref[...] = jnp.sum(gg[...], axis=1)

    @pl.when(is_first)
    def _():
        for peer in range(1, n_stage):
            loss_copy(peer).wait_send()
        loss_ref[0, 0] = loss_src[0, 0]

    @pl.when(jnp.logical_not(is_first))
    def _():
        loss_copy(1).wait_recv()
        loss_ref[0, 0] = loss_dst[0, 0]

    for layer in range(2):
        f_sends = stage < last if layer == 0 else stage > 0
        b_sends = stage < last if layer == 1 else stage > 0
        f_target = jnp.minimum(stage + 1, last) if layer == 0 else jnp.maximum(stage - 1, 0)
        b_target = jnp.minimum(stage + 1, last) if layer == 1 else jnp.maximum(stage - 1, 0)

        @pl.when(f_sends)
        def _():
            for mb in (n_micro - 2, n_micro - 1):
                send_f(layer, mb, f_target).wait_send()

        @pl.when(b_sends)
        def _():
            for mb in (n_micro - 2, n_micro - 1):
                send_b(layer, mb, b_target).wait_send()

        for copy in out_copies(layer):
            copy.wait()


def solution(mesh):
    n_stage = mesh.shape['stage']

    def device_step(tokens, targets, w_in, w_out, norm_gains):
        n_micro, tokens_mb, d_model = tokens.shape
        d_ff = w_in.shape[2]
        any_spec = pl.BlockSpec(memory_space=pl.ANY)
        dma = pltpu.SemaphoreType.DMA
        grad_w_in, grad_w_out_t, grad_gains, loss = pl.pallas_call(
            functools.partial(kernel, n_stage, n_micro),
            out_shape=(jax.ShapeDtypeStruct((2, d_model, d_ff), F32),
                       jax.ShapeDtypeStruct((2, d_model, d_ff), F32),
                       jax.ShapeDtypeStruct((2, d_model), F32),
                       jax.ShapeDtypeStruct((1, 1), F32)),
            in_specs=[any_spec] * 4 + [pl.BlockSpec(memory_space=pltpu.VMEM)],
            out_specs=(any_spec, any_spec, pl.BlockSpec(memory_space=pltpu.VMEM),
                       pl.BlockSpec(memory_space=pltpu.SMEM)),
            scratch_shapes=[
                pltpu.VMEM((2, d_model, d_ff), BF16),
                pltpu.VMEM((2, d_ff, d_model), BF16),
                pltpu.VMEM((2, d_model, d_ff), F32),
                pltpu.VMEM((2, d_model, d_ff), F32),
                pltpu.VMEM((2, 8, d_model), F32),
                pltpu.VMEM((2, n_micro, tokens_mb, d_model), BF16),
                pltpu.VMEM((2, RING, tokens_mb, d_model), BF16),
                pltpu.VMEM((2, 2, tokens_mb, d_model), BF16),
                pltpu.VMEM((2, 2, tokens_mb, d_model), BF16),
                pltpu.VMEM((TGT_SLOTS, tokens_mb, d_model), BF16),
                pltpu.VMEM((tokens_mb, d_ff), BF16),
                pltpu.VMEM((tokens_mb, d_ff), BF16),
                pltpu.VMEM((8, d_model), F32),
                pltpu.VMEM((8, 128), F32),
                pltpu.VMEM((8, 128), F32),
                dma((2, 2)), dma((2, 2)), dma((TGT_SLOTS,)), dma((2, n_micro)), dma((2, RING)),
                dma((2, 2)), dma((2, 2)), pltpu.SemaphoreType.REGULAR((2,)),
                dma((n_stage - 1,)), dma((1,)),
            ],
            compiler_params=pltpu.CompilerParams(
                collective_id=0, has_side_effects=True, vmem_limit_bytes=67043328),
        )(tokens, targets, w_in, w_out, norm_gains)
        return grad_w_in, jnp.swapaxes(grad_w_out_t, 1, 2), grad_gains, loss.reshape(1)

    block_spec = P(('dp', 'stage'))
    return jax.shard_map(device_step, mesh=mesh,
                         in_specs=(P('dp'), P('dp'), P('stage'), P('stage'), P('stage')),
                         out_specs=(block_spec, block_spec, block_spec, P('dp')),
                         check_vma=False)
```

```python
import functools

import jax
import jax.numpy as jnp
from jax import lax
from jax.experimental import pallas as pl
from jax.experimental.pallas import tpu as pltpu
from jax.sharding import PartitionSpec as P

EPSILON = 1e-6
MESH = pl.DeviceIdType.MESH
F32 = jnp.float32
BF16 = jnp.bfloat16
C0 = 0.7978845608028654
C1 = C0 * 0.044715
RING = 8
TOK_AHEAD = 4
TGT_SLOTS = 4
CHUNK = 256
DU_AHEAD = 2
W_LAG = 2
GAP = 1


def dot(lhs, rhs):
    return jnp.dot(lhs, rhs, preferred_element_type=F32)


def dot_t(lhs, rhs):
    return lax.dot_general(lhs, rhs, (((1,), (1,)), ((), ())), preferred_element_type=F32)


def gate(a):
    sq = a * a
    z = a * (C0 + C1 * sq)
    return 0.5 + 0.5 * jnp.tanh(z), sq


def kernel(n_stage, n_micro, tok_hbm, tgt_hbm, wi_hbm, wo_hbm, gain_ref,
           gwi_hbm, gwo_hbm, gg_ref, loss_ref,
           wi, wo, agi, ago, gg, xs, dhs, of, ob, tg, sse, loss_src, loss_dst,
           w_sem, out_sem, tg_sem, rx_sem, rd_sem, sf_sem, sb_sem, free_sem, lsend_sem, lrecv_sem):
    stage = lax.axis_index('stage')
    last = n_stage - 1
    is_first = stage == 0
    is_last = stage == last
    tokens_mb, d_model = xs.shape[2], xs.shape[3]
    d_ff = wi.shape[2]
    seed_scale = 2.0 / (n_micro * tokens_mb)

    barrier = pltpu.get_barrier_semaphore()
    for hop in range(1, n_stage):
        pl.semaphore_signal(barrier, inc=1, device_id={'stage': lax.rem(stage + hop, n_stage)},
                            device_id_type=MESH)
    def weight_copies(layer):
        return (pltpu.make_async_copy(wi_hbm.at[layer], wi.at[layer], w_sem.at[layer, 0]),
                pltpu.make_async_copy(wo_hbm.at[layer], wo.at[layer], w_sem.at[layer, 1]))

    def token_copy(mb):
        return pltpu.make_async_copy(tok_hbm.at[mb], xs.at[0, mb], rx_sem.at[0, mb])

    def target_copy(mb):
        slot = lax.rem(mb, TGT_SLOTS)
        return pltpu.make_async_copy(tgt_hbm.at[mb], tg.at[slot], tg_sem.at[slot])

    def out_copies(layer):
        return (pltpu.make_async_copy(agi.at[layer], gwi_hbm.at[layer], out_sem.at[layer, 0]),
                pltpu.make_async_copy(ago.at[layer], gwo_hbm.at[layer], out_sem.at[layer, 1]))

    for copy in weight_copies(0):
        copy.start()

    @pl.when(is_first)
    def _():
        for mb in range(TOK_AHEAD):
            token_copy(mb).start()

    for copy in weight_copies(1):
        copy.start()

    @pl.when(is_first)
    def _():
        for mb in range(TGT_SLOTS):
            target_copy(mb).start()

    @pl.loop(0, 2 * d_model // 8)
    def _(i):
        layer, row = i // (d_model // 8), lax.rem(i, d_model // 8)
        rows = pl.ds(pl.multiple_of(row * 8, 8), 8)
        agi[layer, rows, :] = jnp.zeros((8, d_ff), F32)
        ago[layer, rows, :] = jnp.zeros((8, d_ff), F32)

    gg[...] = jnp.zeros_like(gg)
    sse[...] = jnp.zeros_like(sse)
    for copy in weight_copies(0):
        copy.wait()
    pl.semaphore_wait(barrier, n_stage - 1)

    def gain_of(layer):
        return jnp.where(layer == 0, gain_ref[0:1, :], gain_ref[1:2, :])

    def fold(rows):
        return jnp.sum(rows.reshape(rows.shape[0] // 8, 8, rows.shape[1]), axis=0)

    def normalize(x, layer):
        inv = lax.rsqrt(jnp.mean(x * x, axis=-1, keepdims=True) + EPSILON)
        xhat = x * inv
        return inv, xhat, (xhat * gain_of(layer)).astype(BF16)

    def compute(layer, mb_f, par_f, mb_b, slot_b, par_b):
        chunks = d_ff // CHUNK
        cols = [pl.ds(c * CHUNK, CHUNK) for c in range(chunks)]
        has_f, has_b = mb_f is not None, mb_b is not None
        du, a_b, a_f, u_b, da_b = {}, {}, {}, {}, {}
        total = dn = None
        if has_b:
            dh = dhs[layer, slot_b]
            for c in range(DU_AHEAD):
                du[c] = dot_t(dh, wo[layer, cols[c], :])
            x_b = xs[layer, mb_b].astype(F32)
            inv_b, xhat_b, normed_b = normalize(x_b, layer)
            a_b[0] = dot(normed_b, wi[layer, :, cols[0]])
        if has_f:
            x_f = xs[layer, mb_f].astype(F32)
            _, _, normed_f = normalize(x_f, layer)
            a_f[0] = dot(normed_f, wi[layer, :, cols[0]])
        if has_b:
            normed_t = normed_b.T
            dh_t = dh.T

        def weight_grads(c):
            agi[layer, :, cols[c]] += dot(normed_t, da_b.pop(c))
            ago[layer, :, cols[c]] += dot(dh_t, u_b.pop(c))

        for c in range(chunks):
            if has_b and c + DU_AHEAD < chunks:
                du[c + DU_AHEAD] = dot_t(dh, wo[layer, cols[c + DU_AHEAD], :])
            if c + 1 < chunks:
                if has_b:
                    a_b[c + 1] = dot(normed_b, wi[layer, :, cols[c + 1]])
                if has_f:
                    a_f[c + 1] = dot(normed_f, wi[layer, :, cols[c + 1]])
            if has_b:
                a = a_b.pop(c)
                q, sq = gate(a)
                u = a * q
                slope = q + u * (1.0 - q) * (2.0 * C0 + 6.0 * C1 * sq)
                da = (du.pop(c) * slope).astype(BF16)
                u_b[c] = u.astype(BF16)
                da_b[c] = da
                part = dot_t(da, wi[layer, :, cols[c]])
                dn = part if dn is None else dn + part
            if has_f:
                a = a_f.pop(c)
                q, _ = gate(a)
                part = dot((a * q).astype(BF16), wo[layer, cols[c], :])
                total = part if total is None else total + part
            if has_b and c >= W_LAG:
                weight_grads(c - W_LAG)
        if has_f:
            of[layer, par_f] = (x_f + total).astype(BF16)
        if has_b:
            weighted = dn * gain_of(layer)
            proj = jnp.mean(weighted * xhat_b, axis=-1, keepdims=True)
            gg[layer] += fold(dn * xhat_b)
            ob[layer, par_b] = (dh.astype(F32) + inv_b * (weighted - xhat_b * proj)).astype(BF16)
            for c in range(chunks - W_LAG, chunks):
                weight_grads(c)

    def send_f(layer, mb, target):
        par = lax.rem(mb, 2)
        return pltpu.make_async_remote_copy(
            src_ref=of.at[layer, par], dst_ref=xs.at[layer, mb],
            send_sem=sf_sem.at[layer, par], recv_sem=rx_sem.at[layer, mb],
            device_id={'stage': target}, device_id_type=MESH)

    def send_b(layer, mb, target):
        par = lax.rem(mb, 2)
        slot = lax.rem(mb, RING)
        return pltpu.make_async_remote_copy(
            src_ref=ob.at[layer, par], dst_ref=dhs.at[layer, slot],
            send_sem=sb_sem.at[layer, par], recv_sem=rd_sem.at[layer, slot],
            device_id={'stage': target}, device_id_type=MESH)

    def plan_f(layer):
        down = layer == 0
        return (jnp.where(down, stage < last, stage > 0), jnp.where(down, True, stage < last),
                jnp.where(down, jnp.minimum(stage + 1, last), jnp.maximum(stage - 1, 0)))

    def plan_b(layer):
        up = layer == 1
        return (jnp.where(up, stage < last, stage > 0), jnp.where(up, stage > 0, stage < last),
                jnp.where(up, jnp.minimum(stage + 1, last), jnp.maximum(stage - 1, 0)),
                jnp.where(up, jnp.maximum(stage - 1, 0), jnp.minimum(stage + 1, last)))

    def begin_f(layer, mb):
        sends, receives, target = plan_f(layer)

        @pl.when((layer == 0) & is_first & (mb + TOK_AHEAD < n_micro))
        def _():
            token_copy(mb + TOK_AHEAD).start()

        @pl.when(receives)
        def _():
            send_f(layer, mb, target).wait_recv()

        @pl.when(sends & (mb >= 2))
        def _():
            send_f(layer, mb - 2, target).wait_send()

    def end_f(layer, mb):
        sends, _, target = plan_f(layer)
        par = lax.rem(mb, 2)

        @pl.when(sends)
        def _():
            send_f(layer, mb, target).start()

        @pl.when((layer == 0) & is_last)
        def _():
            xs[1, mb] = of[0, par]

        @pl.when((layer == 1) & is_first)
        def _():
            target_copy(mb).wait()
            err = of[1, par].astype(F32) - tg[lax.rem(mb, TGT_SLOTS)].astype(F32)
            dhs[1, lax.rem(mb, RING)] = (err * seed_scale).astype(BF16)
            sse[...] += fold(err * err)

            @pl.when(mb + TGT_SLOTS < n_micro)
            def _():
                target_copy(mb + TGT_SLOTS).start()

    def begin_b(layer, mb):
        sends, receives, target, _ = plan_b(layer)

        @pl.when(receives)
        def _():
            send_b(layer, mb, target).wait_recv()

        @pl.when(sends & (mb >= 2))
        def _():
            send_b(layer, mb - 2, target).wait_send()

        @pl.when(sends & (mb >= RING))
        def _():
            pl.semaphore_wait(free_sem.at[layer], 1)

    def end_b(layer, mb):
        sends, receives, target, source = plan_b(layer)

        @pl.when(sends)
        def _():
            send_b(layer, mb, target).start()

        @pl.when((layer == 1) & is_last)
        def _():
            dhs[0, lax.rem(mb, RING)] = ob[1, lax.rem(mb, 2)]

        @pl.when(receives & (mb + RING < n_micro))
        def _():
            pl.semaphore_signal(free_sem.at[layer], inc=1, device_id={'stage': source}, device_id_type=MESH)

        @pl.when(mb == n_micro - 1)
        def _():
            for copy in out_copies(layer):
                copy.start()

    def loss_copy(peer):
        return pltpu.make_async_remote_copy(
            src_ref=loss_src, dst_ref=loss_dst, send_sem=lsend_sem.at[peer - 1], recv_sem=lrecv_sem.at[0],
            device_id={'stage': peer}, device_id_type=MESH)

    gap = GAP if n_stage > 2 else 0
    pos, end = stage + jnp.where(stage >= n_stage // 2, gap, 0), last + gap
    ticks = n_micro + 4 * end + 2

    @pl.loop(0, 2 * ticks)
    def _(step):
        tick, layer = step // 2, lax.rem(step, 2)
        mb_f = tick - jnp.where(layer == 0, pos, 2 * end - pos)
        mb_b = tick - jnp.where(layer == 1, 2 * end + 1 + pos, 4 * end + 2 - pos)
        ok_f = (mb_f >= 0) & (mb_f < n_micro)
        ok_b = (mb_b >= 0) & (mb_b < n_micro)

        @pl.when(step == 1)
        def _():
            for copy in weight_copies(1):
                copy.wait()

        @pl.when(ok_f)
        def _():
            begin_f(layer, mb_f)

        @pl.when(ok_b)
        def _():
            begin_b(layer, mb_b)

        @pl.when(ok_f & ok_b)
        def _():
            compute(layer, mb_f, lax.rem(mb_f, 2), mb_b, lax.rem(mb_b, RING), lax.rem(mb_b, 2))

        @pl.when(ok_f & jnp.logical_not(ok_b))
        def _():
            compute(layer, mb_f, lax.rem(mb_f, 2), None, None, None)

        @pl.when(ok_b & jnp.logical_not(ok_f))
        def _():
            compute(layer, None, None, mb_b, lax.rem(mb_b, RING), lax.rem(mb_b, 2))

        @pl.when(ok_f)
        def _():
            end_f(layer, mb_f)

        @pl.when(ok_b)
        def _():
            end_b(layer, mb_b)

        @pl.when(is_first & (layer == 1) & (mb_f == n_micro - 1))
        def _():
            total = jnp.sum(sse[...]) / (n_micro * tokens_mb * d_model)
            loss_src[...] = jnp.full(loss_src.shape, total, F32)
            for peer in range(1, n_stage):
                loss_copy(peer).start()

    gg_ref[...] = jnp.sum(gg[...], axis=1)

    @pl.when(is_first)
    def _():
        for peer in range(1, n_stage):
            loss_copy(peer).wait_send()
        loss_ref[0, 0] = loss_src[0, 0]

    @pl.when(jnp.logical_not(is_first))
    def _():
        loss_copy(1).wait_recv()
        loss_ref[0, 0] = loss_dst[0, 0]

    for layer in range(2):
        f_sends = stage < last if layer == 0 else stage > 0
        b_sends = stage < last if layer == 1 else stage > 0
        f_target = jnp.minimum(stage + 1, last) if layer == 0 else jnp.maximum(stage - 1, 0)
        b_target = jnp.minimum(stage + 1, last) if layer == 1 else jnp.maximum(stage - 1, 0)

        @pl.when(f_sends)
        def _():
            for mb in (n_micro - 2, n_micro - 1):
                send_f(layer, mb, f_target).wait_send()

        @pl.when(b_sends)
        def _():
            for mb in (n_micro - 2, n_micro - 1):
                send_b(layer, mb, b_target).wait_send()

        for copy in out_copies(layer):
            copy.wait()


def solution(mesh):
    n_stage = mesh.shape['stage']

    def device_step(tokens, targets, w_in, w_out, norm_gains):
        n_micro, tokens_mb, d_model = tokens.shape
        d_ff = w_in.shape[2]
        any_spec = pl.BlockSpec(memory_space=pl.ANY)
        dma = pltpu.SemaphoreType.DMA
        grad_w_in, grad_w_out_t, grad_gains, loss = pl.pallas_call(
            functools.partial(kernel, n_stage, n_micro),
            out_shape=(jax.ShapeDtypeStruct((2, d_model, d_ff), F32),
                       jax.ShapeDtypeStruct((2, d_model, d_ff), F32),
                       jax.ShapeDtypeStruct((2, d_model), F32),
                       jax.ShapeDtypeStruct((1, 1), F32)),
            in_specs=[any_spec] * 4 + [pl.BlockSpec(memory_space=pltpu.VMEM)],
            out_specs=(any_spec, any_spec, pl.BlockSpec(memory_space=pltpu.VMEM),
                       pl.BlockSpec(memory_space=pltpu.SMEM)),
            scratch_shapes=[
                pltpu.VMEM((2, d_model, d_ff), BF16),
                pltpu.VMEM((2, d_ff, d_model), BF16),
                pltpu.VMEM((2, d_model, d_ff), F32),
                pltpu.VMEM((2, d_model, d_ff), F32),
                pltpu.VMEM((2, 8, d_model), F32),
                pltpu.VMEM((2, n_micro, tokens_mb, d_model), BF16),
                pltpu.VMEM((2, RING, tokens_mb, d_model), BF16),
                pltpu.VMEM((2, 2, tokens_mb, d_model), BF16),
                pltpu.VMEM((2, 2, tokens_mb, d_model), BF16),
                pltpu.VMEM((TGT_SLOTS, tokens_mb, d_model), BF16),
                pltpu.VMEM((8, d_model), F32),
                pltpu.VMEM((8, 128), F32),
                pltpu.VMEM((8, 128), F32),
                dma((2, 2)), dma((2, 2)), dma((TGT_SLOTS,)), dma((2, n_micro)), dma((2, RING)),
                dma((2, 2)), dma((2, 2)), pltpu.SemaphoreType.REGULAR((2,)),
                dma((n_stage - 1,)), dma((1,)),
            ],
            compiler_params=pltpu.CompilerParams(
                collective_id=0, has_side_effects=True, vmem_limit_bytes=67043328),
        )(tokens, targets, w_in, w_out, norm_gains)
        return grad_w_in, jnp.swapaxes(grad_w_out_t, 1, 2), grad_gains, loss.reshape(1)

    block_spec = P(('dp', 'stage'))
    return jax.shard_map(device_step, mesh=mesh,
                         in_specs=(P('dp'), P('dp'), P('stage'), P('stage'), P('stage')),
                         out_specs=(block_spec, block_spec, block_spec, P('dp')),
                         check_vma=False)
```

```python
import functools

import jax
import jax.numpy as jnp
from jax import lax
from jax.experimental import pallas as pl
from jax.experimental.pallas import tpu as pltpu
from jax.sharding import PartitionSpec as P

EPSILON = 1e-6
MESH = pl.DeviceIdType.MESH
F32 = jnp.float32
BF16 = jnp.bfloat16
C0 = 0.7978845608028654
C1 = C0 * 0.044715
RING = 4
TOK_AHEAD = 4
TGT_SLOTS = 2
CHUNK = 256
DU_AHEAD = 2
A_AHEAD = 1
W_LAG = 2
GAP = 1
VMEM_LIMIT = 67043328 - 16 * 2**20


def dot(lhs, rhs):
    return jnp.dot(lhs, rhs, preferred_element_type=F32)


def dot_t(lhs, rhs):
    return lax.dot_general(lhs, rhs, (((1,), (1,)), ((), ())), preferred_element_type=F32)


def gate(a):
    sq = a * a
    z = a * (C0 + C1 * sq)
    return 0.5 + 0.5 * jnp.tanh(z), sq


def kernel(n_stage, n_micro, tok_hbm, tgt_hbm, wi_hbm, wo_hbm, gain_ref,
           agi, ago, gg_ref, loss_ref, slope_hbm, hid_hbm,
           wi, wo, gg, xs, dhs, of, ob, tg, slope_out, hid_out, slope_in, hid_in, sse, loss_src, loss_dst,
           w_sem, tg_sem, rx_sem, rd_sem, sf_sem, sb_sem, free_sem, lsend_sem, lrecv_sem, keep_sem, fetch_sem):
    stage = lax.axis_index('stage')
    last = n_stage - 1
    is_first = stage == 0
    is_last = stage == last
    tokens_mb, d_model = xs.shape[2], xs.shape[3]
    d_ff = wi.shape[2]
    seed_scale = 2.0 / (n_micro * tokens_mb)

    barrier = pltpu.get_barrier_semaphore()
    for hop in range(1, n_stage):
        pl.semaphore_signal(barrier, inc=1, device_id={'stage': lax.rem(stage + hop, n_stage)},
                            device_id_type=MESH)
    def weight_copies(layer):
        return (pltpu.make_async_copy(wi_hbm.at[layer], wi.at[layer], w_sem.at[layer, 0]),
                pltpu.make_async_copy(wo_hbm.at[layer], wo.at[layer], w_sem.at[layer, 1]))

    def token_copy(mb):
        return pltpu.make_async_copy(tok_hbm.at[mb], xs.at[0, mb], rx_sem.at[0, mb])

    def target_copy(mb):
        slot = lax.rem(mb, TGT_SLOTS)
        return pltpu.make_async_copy(tgt_hbm.at[mb], tg.at[slot], tg_sem.at[slot])

    for copy in weight_copies(0):
        copy.start()

    @pl.when(is_first)
    def _():
        for mb in range(TOK_AHEAD):
            token_copy(mb).start()

    for copy in weight_copies(1):
        copy.start()

    @pl.when(is_first)
    def _():
        for mb in range(TGT_SLOTS):
            target_copy(mb).start()

    @pl.loop(0, 2 * d_model // 8)
    def _(i):
        layer, row = i // (d_model // 8), lax.rem(i, d_model // 8)
        rows = pl.ds(pl.multiple_of(row * 8, 8), 8)
        agi[layer, rows, :] = jnp.zeros((8, d_ff), F32)

    @pl.loop(0, 2 * d_ff // 32)
    def _(i):
        layer, row = i // (d_ff // 32), lax.rem(i, d_ff // 32)
        ago[layer, pl.ds(pl.multiple_of(row * 32, 32), 32), :] = jnp.zeros((32, d_model), F32)

    gg[...] = jnp.zeros_like(gg)
    sse[...] = jnp.zeros_like(sse)
    for copy in weight_copies(0):
        copy.wait()
    pl.semaphore_wait(barrier, n_stage - 1)

    def gain_of(layer):
        return jnp.where(layer == 0, gain_ref[0:1, :], gain_ref[1:2, :])

    def fold(rows):
        return jnp.sum(rows.reshape(rows.shape[0] // 8, 8, rows.shape[1]), axis=0)

    def normalize(x, layer):
        inv = lax.rsqrt(jnp.mean(x * x, axis=-1, keepdims=True) + EPSILON)
        xhat = x * inv
        return inv, xhat, (xhat * gain_of(layer)).astype(BF16)

    def compute(layer, mb_f, par_f, mb_b, slot_b, par_b):
        chunks = d_ff // CHUNK
        cols = [pl.ds(c * CHUNK, CHUNK) for c in range(chunks)]
        has_f, has_b = mb_f is not None, mb_b is not None
        du, a_f, da_b = {}, {}, {}
        total = dn = None
        if has_b:
            dh = dhs[layer, slot_b]
            for c in range(DU_AHEAD):
                du[c] = dot_t(dh, wo[layer, cols[c], :])
        if has_f:
            x_f = xs[layer, mb_f].astype(F32)
            _, _, normed_f = normalize(x_f, layer)
            for c in range(A_AHEAD):
                a_f[c] = dot(normed_f, wi[layer, :, cols[c]])
        if has_b:
            x_b = xs[layer, mb_b].astype(F32)
            inv_b, xhat_b, normed_b = normalize(x_b, layer)
            normed_t = normed_b.T

        def weight_grads(c):
            agi[layer, :, cols[c]] += dot(normed_t, da_b.pop(c))
            ago[layer, cols[c], :] += dot(hid_in[layer, :, cols[c]].T, dh)

        for c in range(chunks):
            if has_b and c + DU_AHEAD < chunks:
                du[c + DU_AHEAD] = dot_t(dh, wo[layer, cols[c + DU_AHEAD], :])
            if has_f and c + A_AHEAD < chunks:
                a_f[c + A_AHEAD] = dot(normed_f, wi[layer, :, cols[c + A_AHEAD]])
            if has_b:
                da = (du.pop(c) * slope_in[layer, :, cols[c]]).astype(BF16)
                da_b[c] = da
                part = dot_t(da, wi[layer, :, cols[c]])
                dn = part if dn is None else dn + part
            if has_f:
                a = a_f.pop(c)
                q, sq = gate(a)
                u = a * q
                slope_out[layer, :, cols[c]] = q + u * (1.0 - q) * (2.0 * C0 + 6.0 * C1 * sq)
                hid = u.astype(BF16)
                hid_out[layer, :, cols[c]] = hid
                part = dot(hid, wo[layer, cols[c], :])
                total = part if total is None else total + part
            if has_b and c >= W_LAG:
                weight_grads(c - W_LAG)
        if has_f:
            of[layer, par_f] = (x_f + total).astype(BF16)
        if has_b:
            weighted = dn * gain_of(layer)
            proj = jnp.mean(weighted * xhat_b, axis=-1, keepdims=True)
            gg[layer] += fold(dn * xhat_b)
            ob[layer, par_b] = (dh.astype(F32) + inv_b * (weighted - xhat_b * proj)).astype(BF16)
            for c in range(chunks - W_LAG, chunks):
                weight_grads(c)

    def keep_copies(layer, mb):
        return (pltpu.make_async_copy(slope_out.at[layer], slope_hbm.at[layer, mb], keep_sem.at[layer, 0]),
                pltpu.make_async_copy(hid_out.at[layer], hid_hbm.at[layer, mb], keep_sem.at[layer, 1]))

    def fetch_copies(layer, mb):
        return (pltpu.make_async_copy(slope_hbm.at[layer, mb], slope_in.at[layer], fetch_sem.at[layer, 0]),
                pltpu.make_async_copy(hid_hbm.at[layer, mb], hid_in.at[layer], fetch_sem.at[layer, 1]))

    def send_f(layer, mb, target):
        par = lax.rem(mb, 2)
        return pltpu.make_async_remote_copy(
            src_ref=of.at[layer, par], dst_ref=xs.at[layer, mb],
            send_sem=sf_sem.at[layer, par], recv_sem=rx_sem.at[layer, mb],
            device_id={'stage': target}, device_id_type=MESH)

    def send_b(layer, mb, target):
        par = lax.rem(mb, 2)
        slot = lax.rem(mb, RING)
        return pltpu.make_async_remote_copy(
            src_ref=ob.at[layer, par], dst_ref=dhs.at[layer, slot],
            send_sem=sb_sem.at[layer, par], recv_sem=rd_sem.at[layer, slot],
            device_id={'stage': target}, device_id_type=MESH)

    def plan_f(layer):
        down = layer == 0
        return (jnp.where(down, stage < last, stage > 0), jnp.where(down, True, stage < last),
                jnp.where(down, jnp.minimum(stage + 1, last), jnp.maximum(stage - 1, 0)))

    def plan_b(layer):
        up = layer == 1
        return (jnp.where(up, stage < last, stage > 0), jnp.where(up, stage > 0, stage < last),
                jnp.where(up, jnp.minimum(stage + 1, last), jnp.maximum(stage - 1, 0)),
                jnp.where(up, jnp.maximum(stage - 1, 0), jnp.minimum(stage + 1, last)))

    def begin_f(layer, mb):
        sends, receives, target = plan_f(layer)

        @pl.when((layer == 0) & is_first & (mb + TOK_AHEAD < n_micro))
        def _():
            token_copy(mb + TOK_AHEAD).start()

        @pl.when(receives)
        def _():
            send_f(layer, mb, target).wait_recv()

        @pl.when(sends & (mb >= 2))
        def _():
            send_f(layer, mb - 2, target).wait_send()

    def end_f(layer, mb):
        sends, _, target = plan_f(layer)
        par = lax.rem(mb, 2)

        @pl.when(sends)
        def _():
            send_f(layer, mb, target).start()

        @pl.when((layer == 0) & is_last)
        def _():
            xs[1, mb] = of[0, par]

        @pl.when((layer == 1) & is_first)
        def _():
            target_copy(mb).wait()
            err = of[1, par].astype(F32) - tg[lax.rem(mb, TGT_SLOTS)].astype(F32)
            dhs[1, lax.rem(mb, RING)] = (err * seed_scale).astype(BF16)
            sse[...] += fold(err * err)

            @pl.when(mb + TGT_SLOTS < n_micro)
            def _():
                target_copy(mb + TGT_SLOTS).start()

    def begin_b(layer, mb):
        sends, receives, target, _ = plan_b(layer)

        @pl.when(receives)
        def _():
            send_b(layer, mb, target).wait_recv()

        @pl.when(sends & (mb >= 2))
        def _():
            send_b(layer, mb - 2, target).wait_send()

        @pl.when(sends & (mb >= RING))
        def _():
            pl.semaphore_wait(free_sem.at[layer], 1)

    def end_b(layer, mb):
        sends, receives, target, source = plan_b(layer)

        @pl.when(sends)
        def _():
            send_b(layer, mb, target).start()

        @pl.when((layer == 1) & is_last)
        def _():
            dhs[0, lax.rem(mb, RING)] = ob[1, lax.rem(mb, 2)]

        @pl.when(receives & (mb + RING < n_micro))
        def _():
            pl.semaphore_signal(free_sem.at[layer], inc=1, device_id={'stage': source}, device_id_type=MESH)

    def loss_copy(peer):
        return pltpu.make_async_remote_copy(
            src_ref=loss_src, dst_ref=loss_dst, send_sem=lsend_sem.at[peer - 1], recv_sem=lrecv_sem.at[0],
            device_id={'stage': peer}, device_id_type=MESH)

    gap = GAP if n_stage > 2 else 0
    pos, end = stage + jnp.where(stage >= n_stage // 2, gap, 0), last + gap
    ticks = n_micro + 4 * end + 3

    def index_f(tick, layer):
        return tick - jnp.where(layer == 0, pos, 2 * end - pos)

    def index_b(tick, layer):
        return tick - jnp.where(layer == 1, 2 * end + 2 + pos, 4 * end + 3 - pos)

    def inside(mb):
        return (mb >= 0) & (mb < n_micro)

    @pl.loop(0, 2 * ticks)
    def _(step):
        tick, layer = step // 2, lax.rem(step, 2)
        mb_f, mb_b = index_f(tick, layer), index_b(tick, layer)
        ok_f, ok_b = inside(mb_f), inside(mb_b)
        next_b = index_b((step + 1) // 2, 1 - layer)

        @pl.when(step == 1)
        def _():
            for copy in weight_copies(1):
                copy.wait()

        @pl.when(inside(mb_f - 1))
        def _():
            for copy in keep_copies(layer, mb_f - 1):
                copy.wait()

        @pl.when(inside(next_b))
        def _():
            for copy in fetch_copies(1 - layer, next_b):
                copy.start()

        @pl.when(ok_f)
        def _():
            begin_f(layer, mb_f)

        @pl.when(ok_b)
        def _():
            begin_b(layer, mb_b)
            for copy in fetch_copies(layer, mb_b):
                copy.wait()

        @pl.when(ok_f & ok_b)
        def _():
            compute(layer, mb_f, lax.rem(mb_f, 2), mb_b, lax.rem(mb_b, RING), lax.rem(mb_b, 2))

        @pl.when(ok_f & jnp.logical_not(ok_b))
        def _():
            compute(layer, mb_f, lax.rem(mb_f, 2), None, None, None)

        @pl.when(ok_b & jnp.logical_not(ok_f))
        def _():
            compute(layer, None, None, mb_b, lax.rem(mb_b, RING), lax.rem(mb_b, 2))

        @pl.when(ok_f)
        def _():
            end_f(layer, mb_f)

        @pl.when(ok_b)
        def _():
            end_b(layer, mb_b)

        @pl.when(ok_f)
        def _():
            for copy in keep_copies(layer, mb_f):
                copy.start()

        @pl.when(is_first & (layer == 1) & (mb_f == n_micro - 1))
        def _():
            total = jnp.sum(sse[...]) / (n_micro * tokens_mb * d_model)
            loss_src[...] = jnp.full(loss_src.shape, total, F32)
            for peer in range(1, n_stage):
                loss_copy(peer).start()

    gg_ref[...] = jnp.sum(gg[...], axis=1)

    @pl.when(is_first)
    def _():
        for peer in range(1, n_stage):
            loss_copy(peer).wait_send()
        loss_ref[0, 0] = loss_src[0, 0]

    @pl.when(jnp.logical_not(is_first))
    def _():
        loss_copy(1).wait_recv()
        loss_ref[0, 0] = loss_dst[0, 0]

    for layer in range(2):
        f_sends = stage < last if layer == 0 else stage > 0
        b_sends = stage < last if layer == 1 else stage > 0
        f_target = jnp.minimum(stage + 1, last) if layer == 0 else jnp.maximum(stage - 1, 0)
        b_target = jnp.minimum(stage + 1, last) if layer == 1 else jnp.maximum(stage - 1, 0)

        @pl.when(f_sends)
        def _():
            for mb in (n_micro - 2, n_micro - 1):
                send_f(layer, mb, f_target).wait_send()

        @pl.when(b_sends)
        def _():
            for mb in (n_micro - 2, n_micro - 1):
                send_b(layer, mb, b_target).wait_send()


def solution(mesh):
    n_stage = mesh.shape['stage']

    def device_step(tokens, targets, w_in, w_out, norm_gains):
        n_micro, tokens_mb, d_model = tokens.shape
        d_ff = w_in.shape[2]
        any_spec = pl.BlockSpec(memory_space=pl.ANY)
        dma = pltpu.SemaphoreType.DMA
        grad_w_in, grad_w_out, grad_gains, loss, _, _ = pl.pallas_call(
            functools.partial(kernel, n_stage, n_micro),
            out_shape=(pltpu.VMEM((2, d_model, d_ff), F32),
                       pltpu.VMEM((2, d_ff, d_model), F32),
                       jax.ShapeDtypeStruct((2, d_model), F32),
                       jax.ShapeDtypeStruct((1, 1), F32),
                       jax.ShapeDtypeStruct((2, n_micro, tokens_mb, d_ff), F32),
                       jax.ShapeDtypeStruct((2, n_micro, tokens_mb, d_ff), BF16)),
            in_specs=[any_spec] * 4 + [pl.BlockSpec(memory_space=pltpu.VMEM)],
            out_specs=(pl.BlockSpec(memory_space=pltpu.VMEM),) * 3 + (
                       pl.BlockSpec(memory_space=pltpu.SMEM), any_spec, any_spec),
            scratch_shapes=[
                pltpu.VMEM((2, d_model, d_ff), BF16),
                pltpu.VMEM((2, d_ff, d_model), BF16),
                pltpu.VMEM((2, 8, d_model), F32),
                pltpu.VMEM((2, n_micro, tokens_mb, d_model), BF16),
                pltpu.VMEM((2, RING, tokens_mb, d_model), BF16),
                pltpu.VMEM((2, 2, tokens_mb, d_model), BF16),
                pltpu.VMEM((2, 2, tokens_mb, d_model), BF16),
                pltpu.VMEM((TGT_SLOTS, tokens_mb, d_model), BF16),
                pltpu.VMEM((2, tokens_mb, d_ff), F32),
                pltpu.VMEM((2, tokens_mb, d_ff), BF16),
                pltpu.VMEM((2, tokens_mb, d_ff), F32),
                pltpu.VMEM((2, tokens_mb, d_ff), BF16),
                pltpu.VMEM((8, d_model), F32),
                pltpu.VMEM((8, 128), F32),
                pltpu.VMEM((8, 128), F32),
                dma((2, 2)), dma((TGT_SLOTS,)), dma((2, n_micro)), dma((2, RING)),
                dma((2, 2)), dma((2, 2)), pltpu.SemaphoreType.REGULAR((2,)),
                dma((n_stage - 1,)), dma((1,)), dma((2, 2)), dma((2, 2)),
            ],
            compiler_params=pltpu.CompilerParams(
                collective_id=0, has_side_effects=True, vmem_limit_bytes=VMEM_LIMIT),
        )(tokens, targets, w_in, w_out, norm_gains)
        return grad_w_in, grad_w_out, grad_gains, loss.reshape(1)

    block_spec = P(('dp', 'stage'))
    return jax.shard_map(device_step, mesh=mesh,
                         in_specs=(P('dp'), P('dp'), P('stage'), P('stage'), P('stage')),
                         out_specs=(block_spec, block_spec, block_spec, P('dp')),
                         check_vma=False)
```

```python
import functools

import jax
import jax.numpy as jnp
from jax import lax
from jax.experimental import pallas as pl
from jax.experimental.pallas import tpu as pltpu
from jax.sharding import PartitionSpec as P

EPSILON = 1e-6
MESH = pl.DeviceIdType.MESH
F32 = jnp.float32
BF16 = jnp.bfloat16
C0 = 0.7978845608028654
C1 = C0 * 0.044715
RING = 4
TOK_AHEAD = 4
TGT_SLOTS = 2
CHUNK = 256
DU_AHEAD = 2
A_AHEAD = 1
V_AHEAD = 0
W_LAG = 4
GAP_DOWN = 1
GAP_UP = 2
VMEM_LIMIT = 67043328 - 16 * 2**20


def dot(lhs, rhs):
    return jnp.dot(lhs, rhs, preferred_element_type=F32)


def dot_t(lhs, rhs):
    return lax.dot_general(lhs, rhs, (((1,), (1,)), ((), ())), preferred_element_type=F32)


def gate(a):
    sq = a * a
    z = a * (C0 + C1 * sq)
    return 0.5 + 0.5 * jnp.tanh(z), sq


def kernel(n_stage, n_micro, tok_hbm, tgt_hbm, wi_hbm, wo_hbm, gain_ref,
           agi, ago, gg_ref, loss_ref, slope_hbm, hid_hbm,
           wi, wo, gg, xs, dhs, of, ob, tg, slope_out, hid_out, slope_in, hid_in, sse, loss_src, loss_dst,
           w_sem, tg_sem, rx_sem, rd_sem, sf_sem, sb_sem, free_sem, lsend_sem, lrecv_sem, keep_sem, fetch_sem):
    stage = lax.axis_index('stage')
    last = n_stage - 1
    is_first = stage == 0
    is_last = stage == last
    tokens_mb, d_model = xs.shape[2], xs.shape[3]
    d_ff = wi.shape[2]
    seed_scale = 2.0 / (n_micro * tokens_mb)

    barrier = pltpu.get_barrier_semaphore()
    for hop in range(1, n_stage):
        pl.semaphore_signal(barrier, inc=1, device_id={'stage': lax.rem(stage + hop, n_stage)},
                            device_id_type=MESH)
    def weight_copies(layer):
        return (pltpu.make_async_copy(wi_hbm.at[layer], wi.at[layer], w_sem.at[layer, 0]),
                pltpu.make_async_copy(wo_hbm.at[layer], wo.at[layer], w_sem.at[layer, 1]))

    def token_copy(mb):
        return pltpu.make_async_copy(tok_hbm.at[mb], xs.at[0, mb], rx_sem.at[0, mb])

    def target_copy(mb):
        slot = lax.rem(mb, TGT_SLOTS)
        return pltpu.make_async_copy(tgt_hbm.at[mb], tg.at[slot], tg_sem.at[slot])

    for copy in weight_copies(0):
        copy.start()

    @pl.when(is_first)
    def _():
        for mb in range(TOK_AHEAD):
            token_copy(mb).start()

    for copy in weight_copies(1):
        copy.start()

    @pl.when(is_first)
    def _():
        for mb in range(TGT_SLOTS):
            target_copy(mb).start()

    def clear():
        @pl.loop(0, 2 * d_model // 8)
        def _(i):
            layer, row = i // (d_model // 8), lax.rem(i, d_model // 8)
            agi[layer, pl.ds(pl.multiple_of(row * 8, 8), 8), :] = jnp.zeros((8, d_ff), F32)

        @pl.loop(0, 2 * d_ff // 32)
        def _(i):
            layer, row = i // (d_ff // 32), lax.rem(i, d_ff // 32)
            ago[layer, pl.ds(pl.multiple_of(row * 32, 32), 32), :] = jnp.zeros((32, d_model), F32)

    @pl.when(jnp.logical_not(is_first))
    def _():
        clear()

    gg[...] = jnp.zeros_like(gg)
    sse[...] = jnp.zeros_like(sse)
    for copy in weight_copies(0):
        copy.wait()
    pl.semaphore_wait(barrier, n_stage - 1)

    def gain_of(layer):
        return jnp.where(layer == 0, gain_ref[0:1, :], gain_ref[1:2, :])

    def fold(rows):
        return jnp.sum(rows.reshape(rows.shape[0] // 8, 8, rows.shape[1]), axis=0)

    def normalize(x, layer):
        inv = lax.rsqrt(jnp.mean(x * x, axis=-1, keepdims=True) + EPSILON)
        xhat = x * inv
        return inv, xhat, (xhat * gain_of(layer)).astype(BF16)

    def compute(layer, mb_f, par_f, mb_b, slot_b, par_b):
        chunks = d_ff // CHUNK
        cols = [pl.ds(c * CHUNK, CHUNK) for c in range(chunks)]
        has_f, has_b = mb_f is not None, mb_b is not None
        du, a_f, da_b, hid_f, sums = {}, {}, {}, {}, {}
        if has_b:
            dh = dhs[layer, slot_b]
            for c in range(DU_AHEAD):
                du[c] = dot_t(dh, wo[layer, cols[c], :])
        if has_f:
            x_f = xs[layer, mb_f].astype(F32)
            _, _, normed_f = normalize(x_f, layer)
            for c in range(A_AHEAD):
                a_f[c] = dot(normed_f, wi[layer, :, cols[c]])
        if has_b:
            x_b = xs[layer, mb_b].astype(F32)
            inv_b, xhat_b, normed_b = normalize(x_b, layer)
            normed_t = normed_b.T

        def weight_grads(c):
            agi[layer, :, cols[c]] += dot(normed_t, da_b.pop(c))
            ago[layer, cols[c], :] += dot(hid_in[layer, :, cols[c]].T, dh)

        def emit(c):
            if has_b and DU_AHEAD <= c + DU_AHEAD < chunks:
                du[c + DU_AHEAD] = dot_t(dh, wo[layer, cols[c + DU_AHEAD], :])
            if has_f and A_AHEAD <= c + A_AHEAD < chunks:
                a_f[c + A_AHEAD] = dot(normed_f, wi[layer, :, cols[c + A_AHEAD]])
            if has_b and 0 <= c + V_AHEAD < chunks:
                k = c + V_AHEAD
                da_b[k] = (du.pop(k) * slope_in[layer, :, cols[k]]).astype(BF16)
            if has_f and 0 <= c + V_AHEAD < chunks:
                k = c + V_AHEAD
                a = a_f.pop(k)
                q, sq = gate(a)
                u = a * q
                slope_out[layer, :, cols[k]] = q + u * (1.0 - q) * (2.0 * C0 + 6.0 * C1 * sq)
                hid_f[k] = u.astype(BF16)
                hid_out[layer, :, cols[k]] = hid_f[k]
            if has_b and 0 <= c < chunks:
                part = dot_t(da_b[c], wi[layer, :, cols[c]])
                sums['dn'] = sums['dn'] + part if 'dn' in sums else part
            if has_f and 0 <= c < chunks:
                part = dot(hid_f.pop(c), wo[layer, cols[c], :])
                sums['y'] = sums['y'] + part if 'y' in sums else part
            if has_b and 0 <= c - W_LAG < chunks - W_LAG:
                weight_grads(c - W_LAG)

        for c in range(-V_AHEAD, chunks):
            emit(c)
        dn, total = sums.get('dn'), sums.get('y')
        if has_f:
            of[layer, par_f] = (x_f + total).astype(BF16)
        if has_b:
            weighted = dn * gain_of(layer)
            proj = jnp.mean(weighted * xhat_b, axis=-1, keepdims=True)
            gg[layer] += fold(dn * xhat_b)
            ob[layer, par_b] = (dh.astype(F32) + inv_b * (weighted - xhat_b * proj)).astype(BF16)
            for c in range(chunks - W_LAG, chunks):
                weight_grads(c)

    def keep_copies(layer, mb):
        return (pltpu.make_async_copy(slope_out.at[layer], slope_hbm.at[layer, mb], keep_sem.at[layer, 0]),
                pltpu.make_async_copy(hid_out.at[layer], hid_hbm.at[layer, mb], keep_sem.at[layer, 1]))

    def fetch_copies(layer, mb):
        return (pltpu.make_async_copy(slope_hbm.at[layer, mb], slope_in.at[layer], fetch_sem.at[layer, 0]),
                pltpu.make_async_copy(hid_hbm.at[layer, mb], hid_in.at[layer], fetch_sem.at[layer, 1]))

    def send_f(layer, mb, target):
        par = lax.rem(mb, 2)
        return pltpu.make_async_remote_copy(
            src_ref=of.at[layer, par], dst_ref=xs.at[layer, mb],
            send_sem=sf_sem.at[layer, par], recv_sem=rx_sem.at[layer, mb],
            device_id={'stage': target}, device_id_type=MESH)

    def send_b(layer, mb, target):
        par = lax.rem(mb, 2)
        slot = lax.rem(mb, RING)
        return pltpu.make_async_remote_copy(
            src_ref=ob.at[layer, par], dst_ref=dhs.at[layer, slot],
            send_sem=sb_sem.at[layer, par], recv_sem=rd_sem.at[layer, slot],
            device_id={'stage': target}, device_id_type=MESH)

    def plan_f(layer):
        down = layer == 0
        return (jnp.where(down, stage < last, stage > 0), jnp.where(down, True, stage < last),
                jnp.where(down, jnp.minimum(stage + 1, last), jnp.maximum(stage - 1, 0)))

    def plan_b(layer):
        up = layer == 1
        return (jnp.where(up, stage < last, stage > 0), jnp.where(up, stage > 0, stage < last),
                jnp.where(up, jnp.minimum(stage + 1, last), jnp.maximum(stage - 1, 0)),
                jnp.where(up, jnp.maximum(stage - 1, 0), jnp.minimum(stage + 1, last)))

    def begin_f(layer, mb):
        sends, receives, target = plan_f(layer)

        @pl.when((layer == 0) & is_first & (mb + TOK_AHEAD < n_micro))
        def _():
            token_copy(mb + TOK_AHEAD).start()

        @pl.when(receives)
        def _():
            send_f(layer, mb, target).wait_recv()

        @pl.when(sends & (mb >= 2))
        def _():
            send_f(layer, mb - 2, target).wait_send()

    def end_f(layer, mb):
        sends, _, target = plan_f(layer)
        par = lax.rem(mb, 2)

        @pl.when(sends)
        def _():
            send_f(layer, mb, target).start()

        @pl.when((layer == 0) & is_last)
        def _():
            xs[1, mb] = of[0, par]

        @pl.when((layer == 1) & is_first)
        def _():
            target_copy(mb).wait()
            err = of[1, par].astype(F32) - tg[lax.rem(mb, TGT_SLOTS)].astype(F32)
            dhs[1, lax.rem(mb, RING)] = (err * seed_scale).astype(BF16)
            sse[...] += fold(err * err)

            @pl.when(mb + TGT_SLOTS < n_micro)
            def _():
                target_copy(mb + TGT_SLOTS).start()

    def begin_b(layer, mb):
        sends, receives, target, _ = plan_b(layer)

        @pl.when(receives)
        def _():
            send_b(layer, mb, target).wait_recv()

        @pl.when(sends & (mb >= 2))
        def _():
            send_b(layer, mb - 2, target).wait_send()

        @pl.when(sends & (mb >= RING))
        def _():
            pl.semaphore_wait(free_sem.at[layer], 1)

    def end_b(layer, mb):
        sends, receives, target, source = plan_b(layer)

        @pl.when(sends)
        def _():
            send_b(layer, mb, target).start()

        @pl.when((layer == 1) & is_last)
        def _():
            dhs[0, lax.rem(mb, RING)] = ob[1, lax.rem(mb, 2)]

        @pl.when(receives & (mb + RING < n_micro))
        def _():
            pl.semaphore_signal(free_sem.at[layer], inc=1, device_id={'stage': source}, device_id_type=MESH)

    def loss_copy(peer):
        return pltpu.make_async_remote_copy(
            src_ref=loss_src, dst_ref=loss_dst, send_sem=lsend_sem.at[peer - 1], recv_sem=lrecv_sem.at[0],
            device_id={'stage': peer}, device_id_type=MESH)

    far = jnp.where(stage >= n_stage // 2, 1, 0)
    down_at, up_at = stage + GAP_DOWN * far, last - stage + GAP_UP * (1 - far)
    down_len, up_len = last + GAP_DOWN, last + GAP_UP
    ticks = n_micro + 2 * (down_len + up_len) + 3

    def index_f(tick, layer):
        return tick - jnp.where(layer == 0, down_at, down_len + up_at)

    def index_b(tick, layer):
        turn = down_len + up_len + 2
        return tick - jnp.where(layer == 1, turn + down_at, turn + down_len + 1 + up_at)

    def inside(mb):
        return (mb >= 0) & (mb < n_micro)

    @pl.loop(0, 2 * ticks)
    def _(step):
        tick, layer = step // 2, lax.rem(step, 2)
        mb_f, mb_b = index_f(tick, layer), index_b(tick, layer)
        ok_f, ok_b = inside(mb_f), inside(mb_b)
        next_b = index_b((step + 1) // 2, 1 - layer)

        @pl.when(is_first & (layer == 1) & (mb_f == 0))
        def _():
            clear()

        @pl.when(step == 1)
        def _():
            for copy in weight_copies(1):
                copy.wait()

        @pl.when(inside(mb_f - 1))
        def _():
            for copy in keep_copies(layer, mb_f - 1):
                copy.wait()

        @pl.when(inside(next_b))
        def _():
            for copy in fetch_copies(1 - layer, next_b):
                copy.start()

        @pl.when(ok_f)
        def _():
            begin_f(layer, mb_f)

        @pl.when(ok_b)
        def _():
            begin_b(layer, mb_b)
            for copy in fetch_copies(layer, mb_b):
                copy.wait()

        @pl.when(ok_f & ok_b)
        def _():
            compute(layer, mb_f, lax.rem(mb_f, 2), mb_b, lax.rem(mb_b, RING), lax.rem(mb_b, 2))

        @pl.when(ok_f & jnp.logical_not(ok_b))
        def _():
            compute(layer, mb_f, lax.rem(mb_f, 2), None, None, None)

        @pl.when(ok_b & jnp.logical_not(ok_f))
        def _():
            compute(layer, None, None, mb_b, lax.rem(mb_b, RING), lax.rem(mb_b, 2))

        @pl.when(ok_f)
        def _():
            end_f(layer, mb_f)

        @pl.when(ok_b)
        def _():
            end_b(layer, mb_b)

        @pl.when(ok_f)
        def _():
            for copy in keep_copies(layer, mb_f):
                copy.start()

        @pl.when(is_first & (layer == 1) & (mb_f == n_micro - 1))
        def _():
            total = jnp.sum(sse[...]) / (n_micro * tokens_mb * d_model)
            loss_src[...] = jnp.full(loss_src.shape, total, F32)
            for peer in range(1, n_stage):
                loss_copy(peer).start()

    gg_ref[...] = jnp.sum(gg[...], axis=1)

    @pl.when(is_first)
    def _():
        for peer in range(1, n_stage):
            loss_copy(peer).wait_send()
        loss_ref[0, 0] = loss_src[0, 0]

    @pl.when(jnp.logical_not(is_first))
    def _():
        loss_copy(1).wait_recv()
        loss_ref[0, 0] = loss_dst[0, 0]

    for layer in range(2):
        f_sends = stage < last if layer == 0 else stage > 0
        b_sends = stage < last if layer == 1 else stage > 0
        f_target = jnp.minimum(stage + 1, last) if layer == 0 else jnp.maximum(stage - 1, 0)
        b_target = jnp.minimum(stage + 1, last) if layer == 1 else jnp.maximum(stage - 1, 0)

        @pl.when(f_sends)
        def _():
            for mb in (n_micro - 2, n_micro - 1):
                send_f(layer, mb, f_target).wait_send()

        @pl.when(b_sends)
        def _():
            for mb in (n_micro - 2, n_micro - 1):
                send_b(layer, mb, b_target).wait_send()


def solution(mesh):
    n_stage = mesh.shape['stage']

    def device_step(tokens, targets, w_in, w_out, norm_gains):
        n_micro, tokens_mb, d_model = tokens.shape
        d_ff = w_in.shape[2]
        any_spec = pl.BlockSpec(memory_space=pl.ANY)
        dma = pltpu.SemaphoreType.DMA
        grad_w_in, grad_w_out, grad_gains, loss, _, _ = pl.pallas_call(
            functools.partial(kernel, n_stage, n_micro),
            out_shape=(pltpu.VMEM((2, d_model, d_ff), F32),
                       pltpu.VMEM((2, d_ff, d_model), F32),
                       jax.ShapeDtypeStruct((2, d_model), F32),
                       jax.ShapeDtypeStruct((1, 1), F32),
                       jax.ShapeDtypeStruct((2, n_micro, tokens_mb, d_ff), F32),
                       jax.ShapeDtypeStruct((2, n_micro, tokens_mb, d_ff), BF16)),
            in_specs=[any_spec] * 4 + [pl.BlockSpec(memory_space=pltpu.VMEM)],
            out_specs=(pl.BlockSpec(memory_space=pltpu.VMEM),) * 3 + (
                       pl.BlockSpec(memory_space=pltpu.SMEM), any_spec, any_spec),
            scratch_shapes=[
                pltpu.VMEM((2, d_model, d_ff), BF16),
                pltpu.VMEM((2, d_ff, d_model), BF16),
                pltpu.VMEM((2, 8, d_model), F32),
                pltpu.VMEM((2, n_micro, tokens_mb, d_model), BF16),
                pltpu.VMEM((2, RING, tokens_mb, d_model), BF16),
                pltpu.VMEM((2, 2, tokens_mb, d_model), BF16),
                pltpu.VMEM((2, 2, tokens_mb, d_model), BF16),
                pltpu.VMEM((TGT_SLOTS, tokens_mb, d_model), BF16),
                pltpu.VMEM((2, tokens_mb, d_ff), F32),
                pltpu.VMEM((2, tokens_mb, d_ff), BF16),
                pltpu.VMEM((2, tokens_mb, d_ff), F32),
                pltpu.VMEM((2, tokens_mb, d_ff), BF16),
                pltpu.VMEM((8, d_model), F32),
                pltpu.VMEM((8, 128), F32),
                pltpu.VMEM((8, 128), F32),
                dma((2, 2)), dma((TGT_SLOTS,)), dma((2, n_micro)), dma((2, RING)),
                dma((2, 2)), dma((2, 2)), pltpu.SemaphoreType.REGULAR((2,)),
                dma((n_stage - 1,)), dma((1,)), dma((2, 2)), dma((2, 2)),
            ],
            compiler_params=pltpu.CompilerParams(
                collective_id=0, has_side_effects=True, vmem_limit_bytes=VMEM_LIMIT),
        )(tokens, targets, w_in, w_out, norm_gains)
        return grad_w_in, grad_w_out, grad_gains, loss.reshape(1)

    block_spec = P(('dp', 'stage'))
    return jax.shard_map(device_step, mesh=mesh,
                         in_specs=(P('dp'), P('dp'), P('stage'), P('stage'), P('stage')),
                         out_specs=(block_spec, block_spec, block_spec, P('dp')),
                         check_vma=False)
```

```python
import functools

import jax
import jax.numpy as jnp
from jax import lax
from jax.experimental import pallas as pl
from jax.experimental.pallas import tpu as pltpu
from jax.sharding import PartitionSpec as P

EPSILON = 1e-6
MESH = pl.DeviceIdType.MESH
F32 = jnp.float32
BF16 = jnp.bfloat16
C0 = 0.7978845608028654
C1 = C0 * 0.044715
RING = 4
TOK_AHEAD = 4
TGT_SLOTS = 2
CHUNK = 256
DU_AHEAD = 2
A_AHEAD = 1
V_AHEAD = 0
W_LAG = 4
GAP_DOWN = 1
GAP_UP = 1
VMEM_LIMIT = 67043328 - 16 * 2**20


def dot(lhs, rhs):
    return jnp.dot(lhs, rhs, preferred_element_type=F32)


def dot_t(lhs, rhs):
    return lax.dot_general(lhs, rhs, (((1,), (1,)), ((), ())), preferred_element_type=F32)


def gate(a):
    sq = a * a
    z = a * (C0 + C1 * sq)
    return 0.5 + 0.5 * jnp.tanh(z), sq


def kernel(n_stage, n_micro, tok_hbm, tgt_hbm, wi_hbm, wo_hbm, gain_ref,
           agi, ago, gg_ref, loss_ref, slope_hbm, hid_hbm,
           wi, wo, gg, xs, dhs, of, ob, tg, slope_out, hid_out, slope_in, hid_in, sse, loss_src, loss_dst,
           w_sem, tg_sem, rx_sem, rd_sem, sf_sem, sb_sem, free_sem, lsend_sem, lrecv_sem, keep_sem, fetch_sem):
    stage = lax.axis_index('stage')
    last = n_stage - 1
    is_first = stage == 0
    is_last = stage == last
    tokens_mb, d_model = xs.shape[2], xs.shape[3]
    d_ff = wi.shape[2]
    seed_scale = 2.0 / (n_micro * tokens_mb)

    barrier = pltpu.get_barrier_semaphore()
    for hop in range(1, n_stage):
        pl.semaphore_signal(barrier, inc=1, device_id={'stage': lax.rem(stage + hop, n_stage)},
                            device_id_type=MESH)
    def weight_copies(layer):
        return (pltpu.make_async_copy(wi_hbm.at[layer], wi.at[layer], w_sem.at[layer, 0]),
                pltpu.make_async_copy(wo_hbm.at[layer], wo.at[layer], w_sem.at[layer, 1]))

    def token_copy(mb):
        return pltpu.make_async_copy(tok_hbm.at[mb], xs.at[0, mb], rx_sem.at[0, mb])

    def target_copy(mb):
        slot = lax.rem(mb, TGT_SLOTS)
        return pltpu.make_async_copy(tgt_hbm.at[mb], tg.at[slot], tg_sem.at[slot])

    for copy in weight_copies(0):
        copy.start()

    @pl.when(is_first)
    def _():
        for mb in range(TOK_AHEAD):
            token_copy(mb).start()

    for copy in weight_copies(1):
        copy.start()

    @pl.when(is_first)
    def _():
        for mb in range(TGT_SLOTS):
            target_copy(mb).start()

    def clear():
        @pl.loop(0, 2 * d_model // 8)
        def _(i):
            layer, row = i // (d_model // 8), lax.rem(i, d_model // 8)
            agi[layer, pl.ds(pl.multiple_of(row * 8, 8), 8), :] = jnp.zeros((8, d_ff), F32)

        @pl.loop(0, 2 * d_ff // 32)
        def _(i):
            layer, row = i // (d_ff // 32), lax.rem(i, d_ff // 32)
            ago[layer, pl.ds(pl.multiple_of(row * 32, 32), 32), :] = jnp.zeros((32, d_model), F32)

    @pl.when(jnp.logical_not(is_first))
    def _():
        clear()

    gg[...] = jnp.zeros_like(gg)
    sse[...] = jnp.zeros_like(sse)
    for copy in weight_copies(0):
        copy.wait()
    pl.semaphore_wait(barrier, n_stage - 1)

    def gain_of(layer):
        return gain_ref[layer:layer + 1, :]

    def fold(rows):
        return jnp.sum(rows.reshape(rows.shape[0] // 8, 8, rows.shape[1]), axis=0)

    def normalize(x, layer):
        inv = lax.rsqrt(jnp.mean(x * x, axis=-1, keepdims=True) + EPSILON)
        xhat = x * inv
        return inv, xhat, (xhat * gain_of(layer)).astype(BF16)

    def compute(layer, mb_f, par_f, mb_b, slot_b, par_b):
        chunks = d_ff // CHUNK
        cols = [pl.ds(c * CHUNK, CHUNK) for c in range(chunks)]
        has_f, has_b = mb_f is not None, mb_b is not None
        du, a_f, da_b, hid_f, sums = {}, {}, {}, {}, {}
        if has_b:
            dh = dhs[layer, slot_b]
            for c in range(DU_AHEAD):
                du[c] = dot_t(dh, wo[layer, cols[c], :])
        if has_f:
            x_f = xs[layer, mb_f].astype(F32)
            _, _, normed_f = normalize(x_f, layer)
            for c in range(A_AHEAD):
                a_f[c] = dot(normed_f, wi[layer, :, cols[c]])
        if has_b:
            x_b = xs[layer, mb_b].astype(F32)
            inv_b, xhat_b, normed_b = normalize(x_b, layer)
            normed_t = normed_b.T

        def weight_grads(c):
            agi[layer, :, cols[c]] += dot(normed_t, da_b.pop(c))
            ago[layer, cols[c], :] += dot(hid_in[layer, :, cols[c]].T, dh)

        def emit(c):
            if has_b and DU_AHEAD <= c + DU_AHEAD < chunks:
                du[c + DU_AHEAD] = dot_t(dh, wo[layer, cols[c + DU_AHEAD], :])
            if has_f and A_AHEAD <= c + A_AHEAD < chunks:
                a_f[c + A_AHEAD] = dot(normed_f, wi[layer, :, cols[c + A_AHEAD]])
            if has_b and 0 <= c + V_AHEAD < chunks:
                k = c + V_AHEAD
                da_b[k] = (du.pop(k) * slope_in[layer, :, cols[k]]).astype(BF16)
            if has_f and 0 <= c + V_AHEAD < chunks:
                k = c + V_AHEAD
                a = a_f.pop(k)
                q, sq = gate(a)
                u = a * q
                slope_out[layer, :, cols[k]] = q + u * (1.0 - q) * (2.0 * C0 + 6.0 * C1 * sq)
                hid_f[k] = u.astype(BF16)
                hid_out[layer, :, cols[k]] = hid_f[k]
            if has_b and 0 <= c < chunks:
                part = dot_t(da_b[c], wi[layer, :, cols[c]])
                sums['dn'] = sums['dn'] + part if 'dn' in sums else part
            if has_f and 0 <= c < chunks:
                part = dot(hid_f.pop(c), wo[layer, cols[c], :])
                sums['y'] = sums['y'] + part if 'y' in sums else part
            if has_b and 0 <= c - W_LAG < chunks - W_LAG:
                weight_grads(c - W_LAG)

        for c in range(-V_AHEAD, chunks):
            emit(c)
        dn, total = sums.get('dn'), sums.get('y')
        if has_f:
            of[layer, par_f] = (x_f + total).astype(BF16)
        if has_b:
            weighted = dn * gain_of(layer)
            proj = jnp.mean(weighted * xhat_b, axis=-1, keepdims=True)
            gg[layer] += fold(dn * xhat_b)
            ob[layer, par_b] = (dh.astype(F32) + inv_b * (weighted - xhat_b * proj)).astype(BF16)
            for c in range(chunks - W_LAG, chunks):
                weight_grads(c)

    def keep_copies(layer, mb):
        return (pltpu.make_async_copy(slope_out.at[layer], slope_hbm.at[layer, mb], keep_sem.at[layer, 0]),
                pltpu.make_async_copy(hid_out.at[layer], hid_hbm.at[layer, mb], keep_sem.at[layer, 1]))

    def fetch_copies(layer, mb):
        return (pltpu.make_async_copy(slope_hbm.at[layer, mb], slope_in.at[layer], fetch_sem.at[layer, 0]),
                pltpu.make_async_copy(hid_hbm.at[layer, mb], hid_in.at[layer], fetch_sem.at[layer, 1]))

    def send_f(layer, mb, target):
        par = lax.rem(mb, 2)
        return pltpu.make_async_remote_copy(
            src_ref=of.at[layer, par], dst_ref=xs.at[layer, mb],
            send_sem=sf_sem.at[layer, par], recv_sem=rx_sem.at[layer, mb],
            device_id={'stage': target}, device_id_type=MESH)

    def send_b(layer, mb, target):
        par = lax.rem(mb, 2)
        slot = lax.rem(mb, RING)
        return pltpu.make_async_remote_copy(
            src_ref=ob.at[layer, par], dst_ref=dhs.at[layer, slot],
            send_sem=sb_sem.at[layer, par], recv_sem=rd_sem.at[layer, slot],
            device_id={'stage': target}, device_id_type=MESH)

    after, before = jnp.minimum(stage + 1, last), jnp.maximum(stage - 1, 0)

    def plan_f(layer):
        return (stage < last, None, after) if layer == 0 else (stage > 0, stage < last, before)

    def plan_b(layer):
        return (stage < last, stage > 0, after, before) if layer == 1 else (stage > 0, stage < last, before, after)

    def begin_f(layer, mb):
        sends, receives, target = plan_f(layer)

        if layer == 0:
            @pl.when(is_first & (mb + TOK_AHEAD < n_micro))
            def _():
                token_copy(mb + TOK_AHEAD).start()

            send_f(layer, mb, target).wait_recv()
        else:
            @pl.when(receives)
            def _():
                send_f(layer, mb, target).wait_recv()

        @pl.when(sends & (mb >= 2))
        def _():
            send_f(layer, mb - 2, target).wait_send()

    def end_f(layer, mb):
        sends, _, target = plan_f(layer)
        par = lax.rem(mb, 2)

        @pl.when(sends)
        def _():
            send_f(layer, mb, target).start()

        if layer == 0:
            @pl.when(is_last)
            def _():
                xs[1, mb] = of[0, par]

            return

        @pl.when(is_first)
        def _():
            target_copy(mb).wait()
            err = of[1, par].astype(F32) - tg[lax.rem(mb, TGT_SLOTS)].astype(F32)
            dhs[1, lax.rem(mb, RING)] = (err * seed_scale).astype(BF16)
            sse[...] += fold(err * err)

            @pl.when(mb + TGT_SLOTS < n_micro)
            def _():
                target_copy(mb + TGT_SLOTS).start()

    def begin_b(layer, mb):
        sends, receives, target, _ = plan_b(layer)

        @pl.when(receives)
        def _():
            send_b(layer, mb, target).wait_recv()

        @pl.when(sends & (mb >= 2))
        def _():
            send_b(layer, mb - 2, target).wait_send()

        @pl.when(sends & (mb >= RING))
        def _():
            pl.semaphore_wait(free_sem.at[layer], 1)

    def end_b(layer, mb):
        sends, receives, target, source = plan_b(layer)

        @pl.when(sends)
        def _():
            send_b(layer, mb, target).start()

        if layer == 1:
            @pl.when(is_last)
            def _():
                dhs[0, lax.rem(mb, RING)] = ob[1, lax.rem(mb, 2)]

        @pl.when(receives & (mb + RING < n_micro))
        def _():
            pl.semaphore_signal(free_sem.at[layer], inc=1, device_id={'stage': source}, device_id_type=MESH)

    def loss_copy(peer):
        return pltpu.make_async_remote_copy(
            src_ref=loss_src, dst_ref=loss_dst, send_sem=lsend_sem.at[peer - 1], recv_sem=lrecv_sem.at[0],
            device_id={'stage': peer}, device_id_type=MESH)

    far = jnp.where(stage >= n_stage // 2, 1, 0)
    down_at, up_at = stage + GAP_DOWN * far, last - stage + GAP_UP * (1 - far)
    down_len, up_len = last + GAP_DOWN, last + GAP_UP
    ticks = n_micro + 2 * (down_len + up_len) + 3

    def index_f(tick, layer):
        return tick - (down_at if layer == 0 else down_len + up_at)

    def index_b(tick, layer):
        turn = down_len + up_len + 2
        return tick - (turn + down_at if layer == 1 else turn + down_len + 1 + up_at)

    def inside(mb):
        return (mb >= 0) & (mb < n_micro)

    def run_step(tick, layer):
        mb_f, mb_b = index_f(tick, layer), index_b(tick, layer)
        ok_f, ok_b = inside(mb_f), inside(mb_b)
        next_b = index_b(tick + layer, 1 - layer)

        if layer == 1:
            @pl.when(is_first & (mb_f == 0))
            def _():
                clear()

            @pl.when(tick == 0)
            def _():
                for copy in weight_copies(1):
                    copy.wait()

        @pl.when(inside(mb_f - 1))
        def _():
            for copy in keep_copies(layer, mb_f - 1):
                copy.wait()

        @pl.when(inside(next_b))
        def _():
            for copy in fetch_copies(1 - layer, next_b):
                copy.start()

        @pl.when(ok_f)
        def _():
            begin_f(layer, mb_f)

        @pl.when(ok_b)
        def _():
            begin_b(layer, mb_b)
            for copy in fetch_copies(layer, mb_b):
                copy.wait()

        @pl.when(ok_f & ok_b)
        def _():
            compute(layer, mb_f, lax.rem(mb_f, 2), mb_b, lax.rem(mb_b, RING), lax.rem(mb_b, 2))

        @pl.when(ok_f & jnp.logical_not(ok_b))
        def _():
            compute(layer, mb_f, lax.rem(mb_f, 2), None, None, None)

        @pl.when(ok_b & jnp.logical_not(ok_f))
        def _():
            compute(layer, None, None, mb_b, lax.rem(mb_b, RING), lax.rem(mb_b, 2))

        @pl.when(ok_f)
        def _():
            end_f(layer, mb_f)

        @pl.when(ok_b)
        def _():
            end_b(layer, mb_b)

        @pl.when(ok_f)
        def _():
            for copy in keep_copies(layer, mb_f):
                copy.start()

        if layer == 0:
            return

        @pl.when(is_first & (mb_f == n_micro - 1))
        def _():
            total = jnp.sum(sse[...]) / (n_micro * tokens_mb * d_model)
            loss_src[...] = jnp.full(loss_src.shape, total, F32)
            for peer in range(1, n_stage):
                loss_copy(peer).start()

    @pl.loop(0, ticks)
    def _(tick):
        for layer in range(2):
            run_step(tick, layer)

    gg_ref[...] = jnp.sum(gg[...], axis=1)

    @pl.when(is_first)
    def _():
        for peer in range(1, n_stage):
            loss_copy(peer).wait_send()
        loss_ref[0, 0] = loss_src[0, 0]

    @pl.when(jnp.logical_not(is_first))
    def _():
        loss_copy(1).wait_recv()
        loss_ref[0, 0] = loss_dst[0, 0]

    for layer in range(2):
        f_sends = stage < last if layer == 0 else stage > 0
        b_sends = stage < last if layer == 1 else stage > 0
        f_target = jnp.minimum(stage + 1, last) if layer == 0 else jnp.maximum(stage - 1, 0)
        b_target = jnp.minimum(stage + 1, last) if layer == 1 else jnp.maximum(stage - 1, 0)

        @pl.when(f_sends)
        def _():
            for mb in (n_micro - 2, n_micro - 1):
                send_f(layer, mb, f_target).wait_send()

        @pl.when(b_sends)
        def _():
            for mb in (n_micro - 2, n_micro - 1):
                send_b(layer, mb, b_target).wait_send()


def solution(mesh):
    n_stage = mesh.shape['stage']

    def device_step(tokens, targets, w_in, w_out, norm_gains):
        n_micro, tokens_mb, d_model = tokens.shape
        d_ff = w_in.shape[2]
        any_spec = pl.BlockSpec(memory_space=pl.ANY)
        dma = pltpu.SemaphoreType.DMA
        grad_w_in, grad_w_out, grad_gains, loss, _, _ = pl.pallas_call(
            functools.partial(kernel, n_stage, n_micro),
            out_shape=(pltpu.VMEM((2, d_model, d_ff), F32),
                       pltpu.VMEM((2, d_ff, d_model), F32),
                       jax.ShapeDtypeStruct((2, d_model), F32),
                       jax.ShapeDtypeStruct((1, 1), F32),
                       jax.ShapeDtypeStruct((2, n_micro, tokens_mb, d_ff), F32),
                       jax.ShapeDtypeStruct((2, n_micro, tokens_mb, d_ff), BF16)),
            in_specs=[any_spec] * 4 + [pl.BlockSpec(memory_space=pltpu.VMEM)],
            out_specs=(pl.BlockSpec(memory_space=pltpu.VMEM),) * 3 + (
                       pl.BlockSpec(memory_space=pltpu.SMEM), any_spec, any_spec),
            scratch_shapes=[
                pltpu.VMEM((2, d_model, d_ff), BF16),
                pltpu.VMEM((2, d_ff, d_model), BF16),
                pltpu.VMEM((2, 8, d_model), F32),
                pltpu.VMEM((2, n_micro, tokens_mb, d_model), BF16),
                pltpu.VMEM((2, RING, tokens_mb, d_model), BF16),
                pltpu.VMEM((2, 2, tokens_mb, d_model), BF16),
                pltpu.VMEM((2, 2, tokens_mb, d_model), BF16),
                pltpu.VMEM((TGT_SLOTS, tokens_mb, d_model), BF16),
                pltpu.VMEM((2, tokens_mb, d_ff), F32),
                pltpu.VMEM((2, tokens_mb, d_ff), BF16),
                pltpu.VMEM((2, tokens_mb, d_ff), F32),
                pltpu.VMEM((2, tokens_mb, d_ff), BF16),
                pltpu.VMEM((8, d_model), F32),
                pltpu.VMEM((8, 128), F32),
                pltpu.VMEM((8, 128), F32),
                dma((2, 2)), dma((TGT_SLOTS,)), dma((2, n_micro)), dma((2, RING)),
                dma((2, 2)), dma((2, 2)), pltpu.SemaphoreType.REGULAR((2,)),
                dma((n_stage - 1,)), dma((1,)), dma((2, 2)), dma((2, 2)),
            ],
            compiler_params=pltpu.CompilerParams(
                collective_id=0, has_side_effects=True, vmem_limit_bytes=VMEM_LIMIT),
        )(tokens, targets, w_in, w_out, norm_gains)
        return grad_w_in, grad_w_out, grad_gains, loss.reshape(1)

    block_spec = P(('dp', 'stage'))
    return jax.shard_map(device_step, mesh=mesh,
                         in_specs=(P('dp'), P('dp'), P('stage'), P('stage'), P('stage')),
                         out_specs=(block_spec, block_spec, block_spec, P('dp')),
                         check_vma=False)
```

```python
import functools

import jax
import jax.numpy as jnp
from jax import lax
from jax.experimental import pallas as pl
from jax.experimental.pallas import tpu as pltpu
from jax.sharding import PartitionSpec as P

EPSILON = 1e-6
MESH = pl.DeviceIdType.MESH
F32 = jnp.float32
BF16 = jnp.bfloat16
C0 = 0.7978845608028654
C1 = C0 * 0.044715
RING = 8
TOK_AHEAD = 4
TGT_SLOTS = 2
CHUNK = 256
DU_AHEAD = 2
A_AHEAD = 2
V_AHEAD = 0
W_LAG = 3
GAP_DOWN = 1
GAP_UP = 1
VMEM_LIMIT = 67043328 - 16 * 2**20


def dot(lhs, rhs):
    return jnp.dot(lhs, rhs, preferred_element_type=F32)


def dot_t(lhs, rhs):
    return lax.dot_general(lhs, rhs, (((1,), (1,)), ((), ())), preferred_element_type=F32)


def gate(a):
    sq = a * a
    z = a * (C0 + C1 * sq)
    return 0.5 + 0.5 * jnp.tanh(z), sq


def kernel(n_stage, n_micro, tok_hbm, tgt_hbm, wi_hbm, wo_hbm, gain_ref,
           agi, ago, gg_ref, loss_ref, slope_hbm, hid_hbm,
           wi, wo, gg, xs, dhs, of, ob, tg, slope_out, hid_out, slope_in, hid_in, sse, loss_src, loss_dst,
           w_sem, tg_sem, rx_sem, rd_sem, sf_sem, sb_sem, free_sem, lsend_sem, lrecv_sem, keep_sem, fetch_sem):
    stage = lax.axis_index('stage')
    last = n_stage - 1
    is_first = stage == 0
    is_last = stage == last
    tokens_mb, d_model = xs.shape[2], xs.shape[3]
    d_ff = wi.shape[2]
    seed_scale = 2.0 / (n_micro * tokens_mb)

    barrier = pltpu.get_barrier_semaphore()
    for hop in range(1, n_stage):
        pl.semaphore_signal(barrier, inc=1, device_id={'stage': lax.rem(stage + hop, n_stage)},
                            device_id_type=MESH)
    def weight_copies(layer):
        return (pltpu.make_async_copy(wi_hbm.at[layer], wi.at[layer], w_sem.at[layer, 0]),
                pltpu.make_async_copy(wo_hbm.at[layer], wo.at[layer], w_sem.at[layer, 1]))

    def token_copy(mb):
        return pltpu.make_async_copy(tok_hbm.at[mb], xs.at[0, mb], rx_sem.at[0, mb])

    def target_copy(mb):
        slot = lax.rem(mb, TGT_SLOTS)
        return pltpu.make_async_copy(tgt_hbm.at[mb], tg.at[slot], tg_sem.at[slot])

    for copy in weight_copies(0):
        copy.start()

    @pl.when(is_first)
    def _():
        for mb in range(TOK_AHEAD):
            token_copy(mb).start()

    for copy in weight_copies(1):
        copy.start()

    @pl.when(is_first)
    def _():
        for mb in range(TGT_SLOTS):
            target_copy(mb).start()

    def clear():
        @pl.loop(0, 2 * d_model // 8)
        def _(i):
            layer, row = i // (d_model // 8), lax.rem(i, d_model // 8)
            agi[layer, pl.ds(pl.multiple_of(row * 8, 8), 8), :] = jnp.zeros((8, d_ff), F32)

        @pl.loop(0, 2 * d_ff // 32)
        def _(i):
            layer, row = i // (d_ff // 32), lax.rem(i, d_ff // 32)
            ago[layer, pl.ds(pl.multiple_of(row * 32, 32), 32), :] = jnp.zeros((32, d_model), F32)

    @pl.when(jnp.logical_not(is_first))
    def _():
        clear()

    gg[...] = jnp.zeros_like(gg)
    sse[...] = jnp.zeros_like(sse)
    for copy in weight_copies(0):
        copy.wait()
    pl.semaphore_wait(barrier, n_stage - 1)

    def gain_of(layer):
        return gain_ref[layer:layer + 1, :]

    def fold(rows):
        return jnp.sum(rows.reshape(rows.shape[0] // 8, 8, rows.shape[1]), axis=0)

    def normalize(x, layer):
        inv = lax.rsqrt(jnp.mean(x * x, axis=-1, keepdims=True) + EPSILON)
        xhat = x * inv
        return inv, xhat, (xhat * gain_of(layer)).astype(BF16)

    def compute(layer, mb_f, par_f, mb_b, slot_b, par_b):
        chunks = d_ff // CHUNK
        cols = [pl.ds(c * CHUNK, CHUNK) for c in range(chunks)]
        has_f, has_b = mb_f is not None, mb_b is not None
        ahead = A_AHEAD if has_b else 1
        du, a_f, da_b, hid_f, sums = {}, {}, {}, {}, {}
        if has_b:
            dh = dhs[layer, slot_b]
            for c in range(DU_AHEAD):
                du[c] = dot_t(dh, wo[layer, cols[c], :])
        if has_f:
            x_f = xs[layer, mb_f].astype(F32)
            _, _, normed_f = normalize(x_f, layer)
            for c in range(ahead):
                a_f[c] = dot(normed_f, wi[layer, :, cols[c]])
        if has_b:
            x_b = xs[layer, mb_b].astype(F32)
            inv_b, xhat_b, normed_b = normalize(x_b, layer)
            normed_t = normed_b.T

        def weight_grads(c):
            agi[layer, :, cols[c]] += dot(normed_t, da_b.pop(c))
            ago[layer, cols[c], :] += dot(hid_in[layer, :, cols[c]].T, dh)

        def emit(c):
            if has_b and DU_AHEAD <= c + DU_AHEAD < chunks:
                du[c + DU_AHEAD] = dot_t(dh, wo[layer, cols[c + DU_AHEAD], :])
            if has_f and ahead <= c + ahead < chunks:
                a_f[c + ahead] = dot(normed_f, wi[layer, :, cols[c + ahead]])
            if has_b and 0 <= c + V_AHEAD < chunks:
                k = c + V_AHEAD
                da_b[k] = (du.pop(k) * slope_in[layer, :, cols[k]]).astype(BF16)
            if has_f and 0 <= c + V_AHEAD < chunks:
                k = c + V_AHEAD
                a = a_f.pop(k)
                q, sq = gate(a)
                u = a * q
                slope_out[layer, :, cols[k]] = q + u * (1.0 - q) * (2.0 * C0 + 6.0 * C1 * sq)
                hid_f[k] = u.astype(BF16)
                hid_out[layer, :, cols[k]] = hid_f[k]
            if has_b and 0 <= c < chunks:
                part = dot_t(da_b[c], wi[layer, :, cols[c]])
                sums['dn'] = sums['dn'] + part if 'dn' in sums else part
            if has_f and 0 <= c < chunks:
                part = dot(hid_f.pop(c), wo[layer, cols[c], :])
                sums['y'] = sums['y'] + part if 'y' in sums else part
            if has_b and 0 <= c - W_LAG < chunks - W_LAG:
                weight_grads(c - W_LAG)

        for c in range(-V_AHEAD, chunks):
            emit(c)
        dn, total = sums.get('dn'), sums.get('y')
        if has_f:
            of[layer, par_f] = (x_f + total).astype(BF16)
        if has_b:
            weighted = dn * gain_of(layer)
            proj = jnp.mean(weighted * xhat_b, axis=-1, keepdims=True)
            gg[layer] += fold(dn * xhat_b)
            ob[layer, par_b] = (dh.astype(F32) + inv_b * (weighted - xhat_b * proj)).astype(BF16)
            for c in range(chunks - W_LAG, chunks):
                weight_grads(c)

    def keep_copies(layer, mb):
        return (pltpu.make_async_copy(slope_out.at[layer], slope_hbm.at[layer, mb], keep_sem.at[layer, 0]),
                pltpu.make_async_copy(hid_out.at[layer], hid_hbm.at[layer, mb], keep_sem.at[layer, 1]))

    def fetch_copies(layer, mb):
        return (pltpu.make_async_copy(slope_hbm.at[layer, mb], slope_in.at[layer], fetch_sem.at[layer, 0]),
                pltpu.make_async_copy(hid_hbm.at[layer, mb], hid_in.at[layer], fetch_sem.at[layer, 1]))

    def send_f(layer, mb, target):
        par = lax.rem(mb, 2)
        return pltpu.make_async_remote_copy(
            src_ref=of.at[layer, par], dst_ref=xs.at[layer, mb],
            send_sem=sf_sem.at[layer, par], recv_sem=rx_sem.at[layer, mb],
            device_id={'stage': target}, device_id_type=MESH)

    def send_b(layer, mb, target):
        par = lax.rem(mb, 2)
        slot = lax.rem(mb, RING)
        return pltpu.make_async_remote_copy(
            src_ref=ob.at[layer, par], dst_ref=dhs.at[layer, slot],
            send_sem=sb_sem.at[layer, par], recv_sem=rd_sem.at[layer, slot],
            device_id={'stage': target}, device_id_type=MESH)

    after, before = jnp.minimum(stage + 1, last), jnp.maximum(stage - 1, 0)

    def plan_f(layer):
        return (stage < last, None, after) if layer == 0 else (stage > 0, stage < last, before)

    def plan_b(layer):
        return (stage < last, stage > 0, after, before) if layer == 1 else (stage > 0, stage < last, before, after)

    def begin_f(layer, mb):
        sends, receives, target = plan_f(layer)

        if layer == 0:
            @pl.when(is_first & (mb + TOK_AHEAD < n_micro))
            def _():
                token_copy(mb + TOK_AHEAD).start()

            send_f(layer, mb, target).wait_recv()
        else:
            @pl.when(receives)
            def _():
                send_f(layer, mb, target).wait_recv()

        @pl.when(sends & (mb >= 2))
        def _():
            send_f(layer, mb - 2, target).wait_send()

    def end_f(layer, mb):
        sends, _, target = plan_f(layer)
        par = lax.rem(mb, 2)

        @pl.when(sends)
        def _():
            send_f(layer, mb, target).start()

        if layer == 0:
            @pl.when(is_last)
            def _():
                xs[1, mb] = of[0, par]

            return

        @pl.when(is_first)
        def _():
            target_copy(mb).wait()
            err = of[1, par].astype(F32) - tg[lax.rem(mb, TGT_SLOTS)].astype(F32)
            dhs[1, lax.rem(mb, RING)] = (err * seed_scale).astype(BF16)
            sse[...] += fold(err * err)

            @pl.when(mb + TGT_SLOTS < n_micro)
            def _():
                target_copy(mb + TGT_SLOTS).start()

    def begin_b(layer, mb):
        sends, receives, target, _ = plan_b(layer)

        @pl.when(receives)
        def _():
            send_b(layer, mb, target).wait_recv()

        @pl.when(sends & (mb >= 2))
        def _():
            send_b(layer, mb - 2, target).wait_send()

        @pl.when(sends & (mb >= RING))
        def _():
            pl.semaphore_wait(free_sem.at[layer], 1)

    def end_b(layer, mb):
        sends, receives, target, source = plan_b(layer)

        @pl.when(sends)
        def _():
            send_b(layer, mb, target).start()

        if layer == 1:
            @pl.when(is_last)
            def _():
                dhs[0, lax.rem(mb, RING)] = ob[1, lax.rem(mb, 2)]

        @pl.when(receives & (mb + RING < n_micro))
        def _():
            pl.semaphore_signal(free_sem.at[layer], inc=1, device_id={'stage': source}, device_id_type=MESH)

    def loss_copy(peer):
        return pltpu.make_async_remote_copy(
            src_ref=loss_src, dst_ref=loss_dst, send_sem=lsend_sem.at[peer - 1], recv_sem=lrecv_sem.at[0],
            device_id={'stage': peer}, device_id_type=MESH)

    far = jnp.where(stage >= n_stage // 2, 1, 0)
    down_at, up_at = stage + GAP_DOWN * far, last - stage + GAP_UP * (1 - far)
    down_len, up_len = last + GAP_DOWN, last + GAP_UP
    ticks = n_micro + 2 * (down_len + up_len) + 3

    def index_f(tick, layer):
        return tick - (down_at if layer == 0 else down_len + up_at)

    def index_b(tick, layer):
        turn = down_len + up_len + 2
        return tick - (turn + down_at if layer == 1 else turn + down_len + 1 + up_at)

    def inside(mb):
        return (mb >= 0) & (mb < n_micro)

    def run_step(tick, layer):
        mb_f, mb_b = index_f(tick, layer), index_b(tick, layer)
        ok_f, ok_b = inside(mb_f), inside(mb_b)
        next_b = index_b(tick + layer, 1 - layer)

        if layer == 1:
            @pl.when(is_first & (mb_f == 0))
            def _():
                clear()

            @pl.when(tick == 0)
            def _():
                for copy in weight_copies(1):
                    copy.wait()

        @pl.when(inside(mb_f - 1))
        def _():
            for copy in keep_copies(layer, mb_f - 1):
                copy.wait()

        @pl.when(inside(next_b))
        def _():
            for copy in fetch_copies(1 - layer, next_b):
                copy.start()

        @pl.when(ok_f)
        def _():
            begin_f(layer, mb_f)

        @pl.when(ok_b)
        def _():
            begin_b(layer, mb_b)
            for copy in fetch_copies(layer, mb_b):
                copy.wait()

        @pl.when(ok_f & ok_b)
        def _():
            compute(layer, mb_f, lax.rem(mb_f, 2), mb_b, lax.rem(mb_b, RING), lax.rem(mb_b, 2))

        @pl.when(ok_f & jnp.logical_not(ok_b))
        def _():
            compute(layer, mb_f, lax.rem(mb_f, 2), None, None, None)

        @pl.when(ok_b & jnp.logical_not(ok_f))
        def _():
            compute(layer, None, None, mb_b, lax.rem(mb_b, RING), lax.rem(mb_b, 2))

        @pl.when(ok_f)
        def _():
            end_f(layer, mb_f)

        @pl.when(ok_b)
        def _():
            end_b(layer, mb_b)

        @pl.when(ok_f)
        def _():
            for copy in keep_copies(layer, mb_f):
                copy.start()

        if layer == 0:
            return

        @pl.when(is_first & (mb_f == n_micro - 1))
        def _():
            total = jnp.sum(sse[...]) / (n_micro * tokens_mb * d_model)
            loss_src[...] = jnp.full(loss_src.shape, total, F32)
            for peer in range(1, n_stage):
                loss_copy(peer).start()

    @pl.loop(0, ticks)
    def _(tick):
        for layer in range(2):
            run_step(tick, layer)

    gg_ref[...] = jnp.sum(gg[...], axis=1)

    @pl.when(is_first)
    def _():
        for peer in range(1, n_stage):
            loss_copy(peer).wait_send()
        loss_ref[0, 0] = loss_src[0, 0]

    @pl.when(jnp.logical_not(is_first))
    def _():
        loss_copy(1).wait_recv()
        loss_ref[0, 0] = loss_dst[0, 0]

    for layer in range(2):
        f_sends = stage < last if layer == 0 else stage > 0
        b_sends = stage < last if layer == 1 else stage > 0
        f_target = jnp.minimum(stage + 1, last) if layer == 0 else jnp.maximum(stage - 1, 0)
        b_target = jnp.minimum(stage + 1, last) if layer == 1 else jnp.maximum(stage - 1, 0)

        @pl.when(f_sends)
        def _():
            for mb in (n_micro - 2, n_micro - 1):
                send_f(layer, mb, f_target).wait_send()

        @pl.when(b_sends)
        def _():
            for mb in (n_micro - 2, n_micro - 1):
                send_b(layer, mb, b_target).wait_send()


def solution(mesh):
    n_stage = mesh.shape['stage']

    def device_step(tokens, targets, w_in, w_out, norm_gains):
        n_micro, tokens_mb, d_model = tokens.shape
        d_ff = w_in.shape[2]
        any_spec = pl.BlockSpec(memory_space=pl.ANY)
        dma = pltpu.SemaphoreType.DMA
        grad_w_in, grad_w_out, grad_gains, loss, _, _ = pl.pallas_call(
            functools.partial(kernel, n_stage, n_micro),
            out_shape=(pltpu.VMEM((2, d_model, d_ff), F32),
                       pltpu.VMEM((2, d_ff, d_model), F32),
                       jax.ShapeDtypeStruct((2, d_model), F32),
                       jax.ShapeDtypeStruct((1, 1), F32),
                       jax.ShapeDtypeStruct((2, n_micro, tokens_mb, d_ff), F32),
                       jax.ShapeDtypeStruct((2, n_micro, tokens_mb, d_ff), BF16)),
            in_specs=[any_spec] * 4 + [pl.BlockSpec(memory_space=pltpu.VMEM)],
            out_specs=(pl.BlockSpec(memory_space=pltpu.VMEM),) * 3 + (
                       pl.BlockSpec(memory_space=pltpu.SMEM), any_spec, any_spec),
            scratch_shapes=[
                pltpu.VMEM((2, d_model, d_ff), BF16),
                pltpu.VMEM((2, d_ff, d_model), BF16),
                pltpu.VMEM((2, 8, d_model), F32),
                pltpu.VMEM((2, n_micro, tokens_mb, d_model), BF16),
                pltpu.VMEM((2, RING, tokens_mb, d_model), BF16),
                pltpu.VMEM((2, 2, tokens_mb, d_model), BF16),
                pltpu.VMEM((2, 2, tokens_mb, d_model), BF16),
                pltpu.VMEM((TGT_SLOTS, tokens_mb, d_model), BF16),
                pltpu.VMEM((2, tokens_mb, d_ff), F32),
                pltpu.VMEM((2, tokens_mb, d_ff), BF16),
                pltpu.VMEM((2, tokens_mb, d_ff), F32),
                pltpu.VMEM((2, tokens_mb, d_ff), BF16),
                pltpu.VMEM((8, d_model), F32),
                pltpu.VMEM((8, 128), F32),
                pltpu.VMEM((8, 128), F32),
                dma((2, 2)), dma((TGT_SLOTS,)), dma((2, n_micro)), dma((2, RING)),
                dma((2, 2)), dma((2, 2)), pltpu.SemaphoreType.REGULAR((2,)),
                dma((n_stage - 1,)), dma((1,)), dma((2, 2)), dma((2, 2)),
            ],
            compiler_params=pltpu.CompilerParams(
                collective_id=0, has_side_effects=True, vmem_limit_bytes=VMEM_LIMIT),
        )(tokens, targets, w_in, w_out, norm_gains)
        return grad_w_in, grad_w_out, grad_gains, loss.reshape(1)

    block_spec = P(('dp', 'stage'))
    return jax.shard_map(device_step, mesh=mesh,
                         in_specs=(P('dp'), P('dp'), P('stage'), P('stage'), P('stage')),
                         out_specs=(block_spec, block_spec, block_spec, P('dp')),
                         check_vma=False)
```

```python
import functools

import jax
import jax.numpy as jnp
from jax import lax
from jax.experimental import pallas as pl
from jax.experimental.pallas import tpu as pltpu
from jax.sharding import PartitionSpec as P

EPSILON = 1e-6
MESH = pl.DeviceIdType.MESH
F32 = jnp.float32
BF16 = jnp.bfloat16
C0 = 0.7978845608028654
C1 = C0 * 0.044715
RING = 8
TOK_AHEAD = 4
TGT_SLOTS = 2
CHUNK = 256
DU_AHEAD = 2
A_AHEAD = 2
V_AHEAD = 0
W_LAG = 3
GAP_DOWN = 1
GAP_UP = 1
VMEM_LIMIT = 67043328 - 16 * 2**20 - 2**18


def dot(lhs, rhs):
    return jnp.dot(lhs, rhs, preferred_element_type=F32)


def dot_t(lhs, rhs):
    return lax.dot_general(lhs, rhs, (((1,), (1,)), ((), ())), preferred_element_type=F32)


def gate(a):
    sq = a * a
    z = a * (C0 + C1 * sq)
    return 0.5 + 0.5 * jnp.tanh(z), sq


def kernel(n_stage, n_micro, tok_hbm, tgt_hbm, wi_hbm, wo_hbm, gain_hbm,
           agi, ago, gg_ref, loss_ref, slope_hbm, hid_hbm,
           wi, wo, gg, xs, dhs, of, ob, tg, slope_out, hid_out, slope_in, hid_in, sse, loss_src, loss_dst,
           w_sem, tg_sem, rx_sem, rd_sem, sf_sem, sb_sem, free_sem, lsend_sem, lrecv_sem, keep_sem, fetch_sem, gain_ref, gain_sem):
    stage = lax.axis_index('stage')
    last = n_stage - 1
    is_first = stage == 0
    is_last = stage == last
    tokens_mb, d_model = xs.shape[2], xs.shape[3]
    d_ff = wi.shape[2]
    seed_scale = 2.0 / (n_micro * tokens_mb)

    barrier = pltpu.get_barrier_semaphore()
    for hop in range(1, n_stage):
        pl.semaphore_signal(barrier, inc=1, device_id={'stage': lax.rem(stage + hop, n_stage)},
                            device_id_type=MESH)
    def weight_copies(layer):
        return (pltpu.make_async_copy(wi_hbm.at[layer], wi.at[layer], w_sem.at[layer, 0]),
                pltpu.make_async_copy(wo_hbm.at[layer], wo.at[layer], w_sem.at[layer, 1]))

    def token_copy(mb):
        return pltpu.make_async_copy(tok_hbm.at[mb], xs.at[0, mb], rx_sem.at[0, mb])

    def target_copy(mb):
        slot = lax.rem(mb, TGT_SLOTS)
        return pltpu.make_async_copy(tgt_hbm.at[mb], tg.at[slot], tg_sem.at[slot])

    gain_copy = pltpu.make_async_copy(gain_hbm, gain_ref, gain_sem.at[0])
    gain_copy.start()
    for copy in weight_copies(0):
        copy.start()

    @pl.when(is_first)
    def _():
        for mb in range(TOK_AHEAD):
            token_copy(mb).start()

    def clear():
        @pl.loop(0, 2 * d_model // 8)
        def _(i):
            layer, row = i // (d_model // 8), lax.rem(i, d_model // 8)
            agi[layer, pl.ds(pl.multiple_of(row * 8, 8), 8), :] = jnp.zeros((8, d_ff), F32)

        @pl.loop(0, 2 * d_ff // 32)
        def _(i):
            layer, row = i // (d_ff // 32), lax.rem(i, d_ff // 32)
            ago[layer, pl.ds(pl.multiple_of(row * 32, 32), 32), :] = jnp.zeros((32, d_model), F32)

    @pl.when(jnp.logical_not(is_first))
    def _():
        clear()

    gg[...] = jnp.zeros_like(gg)
    sse[...] = jnp.zeros_like(sse)
    gain_copy.wait()
    for copy in weight_copies(0):
        copy.wait()
    for copy in weight_copies(1):
        copy.start()

    @pl.when(is_first)
    def _():
        for mb in range(TGT_SLOTS):
            target_copy(mb).start()

    pl.semaphore_wait(barrier, n_stage - 1)

    def gain_of(layer):
        return gain_ref[layer:layer + 1, :]

    def fold(rows):
        return jnp.sum(rows.reshape(rows.shape[0] // 8, 8, rows.shape[1]), axis=0)

    def normalize(x, layer):
        inv = lax.rsqrt(jnp.mean(x * x, axis=-1, keepdims=True) + EPSILON)
        xhat = x * inv
        return inv, xhat, (xhat * gain_of(layer)).astype(BF16)

    def compute(layer, mb_f, par_f, mb_b, slot_b, par_b):
        chunks = d_ff // CHUNK
        cols = [pl.ds(c * CHUNK, CHUNK) for c in range(chunks)]
        has_f, has_b = mb_f is not None, mb_b is not None
        ahead = A_AHEAD if has_b else 1
        du, a_f, da_b, hid_f, sums = {}, {}, {}, {}, {}
        if has_b:
            dh = dhs[layer, slot_b]
            for c in range(DU_AHEAD):
                du[c] = dot_t(dh, wo[layer, cols[c], :])
        if has_f:
            x_f = xs[layer, mb_f].astype(F32)
            _, _, normed_f = normalize(x_f, layer)
            for c in range(ahead):
                a_f[c] = dot(normed_f, wi[layer, :, cols[c]])
        if has_b:
            x_b = xs[layer, mb_b].astype(F32)
            inv_b, xhat_b, normed_b = normalize(x_b, layer)
            normed_t = normed_b.T

        def weight_grads(c):
            agi[layer, :, cols[c]] += dot(normed_t, da_b.pop(c))
            ago[layer, cols[c], :] += dot(hid_in[layer, :, cols[c]].T, dh)

        def emit(c):
            if has_b and DU_AHEAD <= c + DU_AHEAD < chunks:
                du[c + DU_AHEAD] = dot_t(dh, wo[layer, cols[c + DU_AHEAD], :])
            if has_f and ahead <= c + ahead < chunks:
                a_f[c + ahead] = dot(normed_f, wi[layer, :, cols[c + ahead]])
            if has_b and 0 <= c + V_AHEAD < chunks:
                k = c + V_AHEAD
                da_b[k] = (du.pop(k) * slope_in[layer, :, cols[k]]).astype(BF16)
            if has_f and 0 <= c + V_AHEAD < chunks:
                k = c + V_AHEAD
                a = a_f.pop(k)
                q, sq = gate(a)
                u = a * q
                slope_out[layer, :, cols[k]] = q + u * (1.0 - q) * (2.0 * C0 + 6.0 * C1 * sq)
                hid_f[k] = u.astype(BF16)
                hid_out[layer, :, cols[k]] = hid_f[k]
            if has_b and 0 <= c < chunks:
                part = dot_t(da_b[c], wi[layer, :, cols[c]])
                sums['dn'] = sums['dn'] + part if 'dn' in sums else part
            if has_f and 0 <= c < chunks:
                part = dot(hid_f.pop(c), wo[layer, cols[c], :])
                sums['y'] = sums['y'] + part if 'y' in sums else part
            if has_b and 0 <= c - W_LAG < chunks - W_LAG:
                weight_grads(c - W_LAG)

        for c in range(-V_AHEAD, chunks):
            emit(c)
        dn, total = sums.get('dn'), sums.get('y')
        if has_f:
            of[layer, par_f] = (x_f + total).astype(BF16)
        if has_b:
            weighted = dn * gain_of(layer)
            proj = jnp.mean(weighted * xhat_b, axis=-1, keepdims=True)
            gg[layer] += fold(dn * xhat_b)
            ob[layer, par_b] = (dh.astype(F32) + inv_b * (weighted - xhat_b * proj)).astype(BF16)
            for c in range(chunks - W_LAG, chunks):
                weight_grads(c)

    def keep_copies(layer, mb):
        return (pltpu.make_async_copy(slope_out.at[layer], slope_hbm.at[layer, mb], keep_sem.at[layer, 0]),
                pltpu.make_async_copy(hid_out.at[layer], hid_hbm.at[layer, mb], keep_sem.at[layer, 1]))

    def fetch_copies(layer, mb):
        return (pltpu.make_async_copy(slope_hbm.at[layer, mb], slope_in.at[layer], fetch_sem.at[layer, 0]),
                pltpu.make_async_copy(hid_hbm.at[layer, mb], hid_in.at[layer], fetch_sem.at[layer, 1]))

    def send_f(layer, mb, target):
        par = lax.rem(mb, 2)
        return pltpu.make_async_remote_copy(
            src_ref=of.at[layer, par], dst_ref=xs.at[layer, mb],
            send_sem=sf_sem.at[layer, par], recv_sem=rx_sem.at[layer, mb],
            device_id={'stage': target}, device_id_type=MESH)

    def send_b(layer, mb, target):
        par = lax.rem(mb, 2)
        slot = lax.rem(mb, RING)
        return pltpu.make_async_remote_copy(
            src_ref=ob.at[layer, par], dst_ref=dhs.at[layer, slot],
            send_sem=sb_sem.at[layer, par], recv_sem=rd_sem.at[layer, slot],
            device_id={'stage': target}, device_id_type=MESH)

    after, before = jnp.minimum(stage + 1, last), jnp.maximum(stage - 1, 0)

    def plan_f(layer):
        return (stage < last, None, after) if layer == 0 else (stage > 0, stage < last, before)

    def plan_b(layer):
        return (stage < last, stage > 0, after, before) if layer == 1 else (stage > 0, stage < last, before, after)

    def begin_f(layer, mb):
        sends, receives, target = plan_f(layer)

        if layer == 0:
            @pl.when(is_first & (mb + TOK_AHEAD < n_micro))
            def _():
                token_copy(mb + TOK_AHEAD).start()

            send_f(layer, mb, target).wait_recv()
        else:
            @pl.when(receives)
            def _():
                send_f(layer, mb, target).wait_recv()

        @pl.when(sends & (mb >= 2))
        def _():
            send_f(layer, mb - 2, target).wait_send()

    def end_f(layer, mb):
        sends, _, target = plan_f(layer)
        par = lax.rem(mb, 2)

        @pl.when(sends)
        def _():
            send_f(layer, mb, target).start()

        if layer == 0:
            @pl.when(is_last)
            def _():
                xs[1, mb] = of[0, par]

            return

        @pl.when(is_first)
        def _():
            target_copy(mb).wait()
            err = of[1, par].astype(F32) - tg[lax.rem(mb, TGT_SLOTS)].astype(F32)
            dhs[1, lax.rem(mb, RING)] = (err * seed_scale).astype(BF16)
            sse[...] += fold(err * err)

            @pl.when(mb + TGT_SLOTS < n_micro)
            def _():
                target_copy(mb + TGT_SLOTS).start()

    def begin_b(layer, mb):
        sends, receives, target, _ = plan_b(layer)

        @pl.when(receives)
        def _():
            send_b(layer, mb, target).wait_recv()

        @pl.when(sends & (mb >= 2))
        def _():
            send_b(layer, mb - 2, target).wait_send()

        @pl.when(sends & (mb >= RING))
        def _():
            pl.semaphore_wait(free_sem.at[layer], 1)

    def end_b(layer, mb):
        sends, receives, target, source = plan_b(layer)

        @pl.when(sends)
        def _():
            send_b(layer, mb, target).start()

        if layer == 1:
            @pl.when(is_last)
            def _():
                dhs[0, lax.rem(mb, RING)] = ob[1, lax.rem(mb, 2)]

        @pl.when(receives & (mb + RING < n_micro))
        def _():
            pl.semaphore_signal(free_sem.at[layer], inc=1, device_id={'stage': source}, device_id_type=MESH)

    def loss_copy(peer):
        return pltpu.make_async_remote_copy(
            src_ref=loss_src, dst_ref=loss_dst, send_sem=lsend_sem.at[peer - 1], recv_sem=lrecv_sem.at[0],
            device_id={'stage': peer}, device_id_type=MESH)

    far = jnp.where(stage >= n_stage // 2, 1, 0)
    down_at, up_at = stage + GAP_DOWN * far, last - stage + GAP_UP * (1 - far)
    down_len, up_len = last + GAP_DOWN, last + GAP_UP
    ticks = n_micro + 2 * (down_len + up_len) + 3

    def index_f(tick, layer):
        return tick - (down_at if layer == 0 else down_len + up_at)

    def index_b(tick, layer):
        turn = down_len + up_len + 2
        return tick - (turn + down_at if layer == 1 else turn + down_len + 1 + up_at)

    def inside(mb):
        return (mb >= 0) & (mb < n_micro)

    def run_step(tick, layer):
        mb_f, mb_b = index_f(tick, layer), index_b(tick, layer)
        ok_f, ok_b = inside(mb_f), inside(mb_b)
        next_b = index_b(tick + layer, 1 - layer)

        if layer == 1:
            @pl.when(is_first & (mb_f == 0))
            def _():
                clear()

            @pl.when(tick == 0)
            def _():
                for copy in weight_copies(1):
                    copy.wait()

        @pl.when(inside(mb_f - 1))
        def _():
            for copy in keep_copies(layer, mb_f - 1):
                copy.wait()

        @pl.when(inside(next_b))
        def _():
            for copy in fetch_copies(1 - layer, next_b):
                copy.start()

        @pl.when(ok_f)
        def _():
            begin_f(layer, mb_f)

        @pl.when(ok_b)
        def _():
            begin_b(layer, mb_b)
            for copy in fetch_copies(layer, mb_b):
                copy.wait()

        @pl.when(ok_f & ok_b)
        def _():
            compute(layer, mb_f, lax.rem(mb_f, 2), mb_b, lax.rem(mb_b, RING), lax.rem(mb_b, 2))

        @pl.when(ok_f & jnp.logical_not(ok_b))
        def _():
            compute(layer, mb_f, lax.rem(mb_f, 2), None, None, None)

        @pl.when(ok_b & jnp.logical_not(ok_f))
        def _():
            compute(layer, None, None, mb_b, lax.rem(mb_b, RING), lax.rem(mb_b, 2))

        @pl.when(ok_f)
        def _():
            end_f(layer, mb_f)

        @pl.when(ok_b)
        def _():
            end_b(layer, mb_b)

        @pl.when(ok_f)
        def _():
            for copy in keep_copies(layer, mb_f):
                copy.start()

        if layer == 0:
            return

        @pl.when(is_first & (mb_f == n_micro - 1))
        def _():
            total = jnp.sum(sse[...]) / (n_micro * tokens_mb * d_model)
            loss_src[...] = jnp.full(loss_src.shape, total, F32)
            for peer in range(1, n_stage):
                loss_copy(peer).start()

    @pl.loop(0, ticks)
    def _(tick):
        for layer in range(2):
            run_step(tick, layer)

    gg_ref[...] = jnp.sum(gg[...], axis=1)

    @pl.when(is_first)
    def _():
        for peer in range(1, n_stage):
            loss_copy(peer).wait_send()
        loss_ref[0, 0] = loss_src[0, 0]

    @pl.when(jnp.logical_not(is_first))
    def _():
        loss_copy(1).wait_recv()
        loss_ref[0, 0] = loss_dst[0, 0]

    for layer in range(2):
        f_sends = stage < last if layer == 0 else stage > 0
        b_sends = stage < last if layer == 1 else stage > 0
        f_target = jnp.minimum(stage + 1, last) if layer == 0 else jnp.maximum(stage - 1, 0)
        b_target = jnp.minimum(stage + 1, last) if layer == 1 else jnp.maximum(stage - 1, 0)

        @pl.when(f_sends)
        def _():
            for mb in (n_micro - 2, n_micro - 1):
                send_f(layer, mb, f_target).wait_send()

        @pl.when(b_sends)
        def _():
            for mb in (n_micro - 2, n_micro - 1):
                send_b(layer, mb, b_target).wait_send()


def solution(mesh):
    n_stage = mesh.shape['stage']

    def device_step(tokens, targets, w_in, w_out, norm_gains):
        n_micro, tokens_mb, d_model = tokens.shape
        d_ff = w_in.shape[2]
        any_spec = pl.BlockSpec(memory_space=pl.ANY)
        dma = pltpu.SemaphoreType.DMA
        grad_w_in, grad_w_out, grad_gains, loss, _, _ = pl.pallas_call(
            functools.partial(kernel, n_stage, n_micro),
            out_shape=(pltpu.VMEM((2, d_model, d_ff), F32),
                       pltpu.VMEM((2, d_ff, d_model), F32),
                       pltpu.VMEM((2, d_model), F32),
                       jax.ShapeDtypeStruct((1, 1), F32),
                       jax.ShapeDtypeStruct((2, n_micro, tokens_mb, d_ff), F32),
                       jax.ShapeDtypeStruct((2, n_micro, tokens_mb, d_ff), BF16)),
            in_specs=[any_spec] * 5,
            out_specs=(pl.BlockSpec(memory_space=pltpu.VMEM),) * 3 + (
                       pl.BlockSpec(memory_space=pltpu.SMEM), any_spec, any_spec),
            scratch_shapes=[
                pltpu.VMEM((2, d_model, d_ff), BF16),
                pltpu.VMEM((2, d_ff, d_model), BF16),
                pltpu.VMEM((2, 8, d_model), F32),
                pltpu.VMEM((2, n_micro, tokens_mb, d_model), BF16),
                pltpu.VMEM((2, RING, tokens_mb, d_model), BF16),
                pltpu.VMEM((2, 2, tokens_mb, d_model), BF16),
                pltpu.VMEM((2, 2, tokens_mb, d_model), BF16),
                pltpu.VMEM((TGT_SLOTS, tokens_mb, d_model), BF16),
                pltpu.VMEM((2, tokens_mb, d_ff), F32),
                pltpu.VMEM((2, tokens_mb, d_ff), BF16),
                pltpu.VMEM((2, tokens_mb, d_ff), F32),
                pltpu.VMEM((2, tokens_mb, d_ff), BF16),
                pltpu.VMEM((8, d_model), F32),
                pltpu.VMEM((8, 128), F32),
                pltpu.VMEM((8, 128), F32),
                dma((2, 2)), dma((TGT_SLOTS,)), dma((2, n_micro)), dma((2, RING)),
                dma((2, 2)), dma((2, 2)), pltpu.SemaphoreType.REGULAR((2,)),
                dma((n_stage - 1,)), dma((1,)), dma((2, 2)), dma((2, 2)),
                pltpu.VMEM((2, d_model), F32), dma((1,)),
            ],
            compiler_params=pltpu.CompilerParams(
                collective_id=0, has_side_effects=True, vmem_limit_bytes=VMEM_LIMIT),
        )(tokens, targets, w_in, w_out, norm_gains)
        return grad_w_in, grad_w_out, grad_gains, loss.reshape(1)

    block_spec = P(('dp', 'stage'))
    return jax.shard_map(device_step, mesh=mesh,
                         in_specs=(P('dp'), P('dp'), P('stage'), P('stage'), P('stage')),
                         out_specs=(block_spec, block_spec, block_spec, P('dp')),
                         check_vma=False)
```
